256 devices in a mesh: row: 2 (over y_hi), circ: 16 (over x, y_lo, core), span: 8 (over z).
Axes of the slice: x: 4, y: 4 (y_hi: 2, y_lo: 2; y = y_hi * 2 + y_lo), z: 8, core: 2. Of those that a mesh axis runs over, the one named last changes fastest.
Arguments:
- density: float32 [2, 128, 128, 256], P('row', 'circ', 'span'), may hold values from 0.6 to 1.6
- velocity: float32 [2, 3, 128, 128, 256], P('row', None, 'circ', 'span'), may hold values from -1.2 to 1.2
- pressure: float32 [2, 128, 128, 256], P('row', 'circ', 'span'), may hold values from 0.6 to 1.6
- blade_force: float32 [2, 3, 128, 128, 256], P('row', None, 'circ', 'span'), may hold values from -4 to 4
- offsets: int32 [2], replicated, may hold values from 0 to 127
- weights: float32 [2, 4], replicated, may hold values from 0.1 to 1
Outputs:
- state: float32 [2, 5, 128, 128, 256], P('row', None, 'circ', 'span')
- plane_flux: float32 [2, 2, 5, 128, 128], P('row', None, None, 'circ', 'span')
The draws below stay inside these ranges and needn't reach their ends.
All inputs are finite; a program needn't handle non-finite values.
Results may differ from the reference program's by a relative error of at most 0.0003.
Values sent between devices are 32-bit elements; how exact they have to be, the bound alone decides.
A program may use at most 64 MiB of HBM per device.

```python
import math
import jax
import jax.numpy as jnp
from jax import lax

C_DEV = 8
NA = 256
STEPS = 2
NC = 128
NS = 128


def shard_levels(own_key, dims, shards, least, largest):
    def one(position, parts):
        heights = jax.random.uniform(jax.random.fold_in(jax.random.fold_in(own_key, 6), position), (parts,), jnp.float32, least / len(shards), largest / len(shards))
        return jnp.repeat(jnp.exp(heights), dims[position] // parts).reshape((-1,) + (1,) * (len(dims) - position - 1))

    loudness = one(*shards[0])
    for cut in shards[1:]:
        loudness = loudness * one(*cut)
    return loudness


def scatter_about(stream_key, extent, scale, most, pieces=(), kind=jnp.bfloat16):
    loudness = shard_levels(stream_key, extent, pieces, -0.22, 0.18) if pieces else 1.0
    result = jax.random.normal(stream_key, extent, jnp.float32) * scale * loudness
    return jnp.minimum(jnp.maximum(result, -most), most).astype(kind)


def setup_inputs(seed: int = 0) -> dict:
    keys = jax.random.split(jax.random.key(seed), 7)
    density = jnp.clip(jnp.exp(math.log(1.6) - 0.98082923 * jax.random.uniform(keys[0], (2, NC, NS, NA), jnp.float32) ** shard_levels(keys[0], (2, NC, NS, NA), ((0, 2), (1, 16), (2, 8)), -0.2, 0.2)), 0.6, 1.6)
    velocity = scatter_about(keys[1], (2, 3, NC, NS, NA), 0.3, 1.2, ((0, 2), (2, 16), (3, 8)), jnp.float32)
    pressure = jnp.clip(jnp.exp(math.log(1.6) - 0.98082923 * jax.random.uniform(keys[2], (2, NC, NS, NA), jnp.float32) ** shard_levels(keys[2], (2, NC, NS, NA), ((0, 2), (1, 16), (2, 8)), -0.2, 0.2)), 0.6, 1.6)
    blade_force = scatter_about(keys[3], (2, 3, NC, NS, NA), 1.0, 4.0, ((0, 2), (2, 16), (3, 8)), jnp.float32)
    offsets = jax.random.randint(keys[4], (STEPS,), 0, NC).astype(jnp.int32)
    weights = jnp.clip(jax.random.uniform(keys[5], (STEPS, 4), jnp.float32, 0.1, 1.0), 0.1, 1.0)
    return {"density": density, "velocity": velocity, "pressure": pressure, "blade_force": blade_force, "offsets": offsets, "weights": weights}


HEAT_RATIO = 1.4
TIME_STEP = 0.04

def direction_flux(cells, direction):
    density_here = cells[0]
    momentum = cells[1:4]
    energy = cells[4]
    kinetic = 0.5 * (momentum[0] * momentum[0] + momentum[1] * momentum[1] + momentum[2] * momentum[2]) / density_here
    pressure_now = (HEAT_RATIO - 1.0) * (energy - kinetic)
    normal = momentum[direction] / density_here
    components = [momentum[direction], momentum[0] * normal, momentum[1] * normal, momentum[2] * normal, (energy + pressure_now) * normal]
    components[1 + direction] = components[1 + direction] + pressure_now
    wave_speed = jnp.abs(normal) + jnp.sqrt(HEAT_RATIO * pressure_now / density_here)
    return (jnp.stack(components), wave_speed)

def face_flux(left_state, right_state, direction):
    left_flux, left_speed = direction_flux(left_state, direction)
    right_flux, right_speed = direction_flux(right_state, direction)
    top_speed = jnp.maximum(left_speed, right_speed)
    return 0.5 * (left_flux + right_flux) - 0.5 * top_speed * (right_state - left_state)

def region_step(padded, force, lower_ghost, upper_ghost):
    region = padded[:, 1:-1, 1:-1]
    circ_flux = face_flux(padded[:, :-1, 1:-1], padded[:, 1:, 1:-1], 1)
    span_flux = face_flux(padded[:, 1:-1, :-1], padded[:, 1:-1, 1:], 2)
    axial_row = jnp.concatenate([lower_ghost, region, upper_ghost], 3)
    axial_flux = face_flux(axial_row[..., :-1], axial_row[..., 1:], 0)
    divergence = axial_flux[..., 1:] - axial_flux[..., :-1] + (circ_flux[:, 1:] - circ_flux[:, :-1]) + (span_flux[:, :, 1:] - span_flux[:, :, :-1])
    source = jnp.stack([jnp.zeros_like(region[0]), region[0] * force[0], region[0] * force[1], region[0] * force[2], lax.optimization_barrier(jnp.sum(region[1:4] * force, axis=0))])
    updated = region - TIME_STEP * divergence + TIME_STEP * source
    return (updated, axial_flux[..., 0], axial_flux[..., -1])

def conserved(density_row, velocity_row, pressure_row):
    momentum = density_row[None] * velocity_row
    energy = pressure_row / (HEAT_RATIO - 1.0) + 0.5 * density_row * lax.optimization_barrier(jnp.sum(velocity_row * velocity_row, axis=0))
    return jnp.concatenate([density_row[None], momentum, energy[None]], 0)

def mirror_sign():
    return jnp.array([1.0, 1.0, 1.0, -1.0, 1.0], jnp.float32).reshape(5, 1, 1, 1)

def advance_row(cells, force, lower_ghost, upper_ghost, row_index):
    flip_sign = mirror_sign()
    wrapped = jnp.concatenate([cells[:, -1:], cells, cells[:, :1]], 1)
    padded = jnp.concatenate([wrapped[:, :, :1] * flip_sign, wrapped, wrapped[:, :, -1:] * flip_sign], 2)
    block_count = NC // C_DEV

    def one_block(block_index):
        start = (block_index * C_DEV).astype(jnp.int32)
        piece = lax.dynamic_slice_in_dim(padded, start, C_DEV + 2, 1)
        force_piece = lax.dynamic_slice_in_dim(force, start, C_DEV, 1)
        lower_piece = lax.dynamic_slice_in_dim(lower_ghost, start, C_DEV, 1)
        upper_piece = lax.dynamic_slice_in_dim(upper_ghost, start, C_DEV, 1)
        updated, first_face, last_face = region_step(piece, force_piece, lower_piece, upper_piece)
        plane = last_face if row_index == 0 else first_face
        return (updated, plane)
    blocks, planes = lax.map(one_block, jnp.arange(block_count, dtype=jnp.int32))
    updated = jnp.moveaxis(blocks, 0, 1).reshape(5, NC, NS, NA)
    plane = jnp.moveaxis(planes, 0, 1).reshape(5, NC, NS)
    return (updated, plane)

def reference(density, velocity, pressure, blade_force, offsets, weights):
    states = [conserved(density[0], velocity[0], pressure[0]), conserved(density[1], velocity[1], pressure[1])]
    tap_weights = weights / lax.optimization_barrier(jnp.sum(weights, axis=1, keepdims=True))
    inlet = jnp.array([1.0, 0.5, 0.0, 0.0, 2.625], jnp.float32).reshape(5, 1, 1, 1)
    planes = [[], []]
    for step_index in range(STEPS):
        turn = offsets[step_index].astype(jnp.int32)
        shifts = [turn, (NC - turn) % NC]
        donors = [states[1][..., 0], states[0][..., -1]]
        updated_rows = []
        for row_index in range(2):
            cells = states[row_index]
            ghost_layer = jnp.zeros_like(donors[row_index])
            for tap_index in range(4):
                ghost_layer = ghost_layer + tap_weights[step_index, tap_index] * jnp.roll(donors[row_index], -(shifts[row_index] + tap_index - 1), axis=1)
            ghost_layer = ghost_layer[..., None]
            if row_index == 0:
                lower_ghost = jnp.broadcast_to(inlet, ghost_layer.shape)
                upper_ghost = ghost_layer
            else:
                lower_ghost = ghost_layer
                upper_ghost = cells[..., -1:]
            updated, plane = advance_row(cells, blade_force[row_index], lower_ghost, upper_ghost, row_index)
            updated_rows.append(updated)
            planes[row_index].append(plane)
        states = updated_rows
    state = jnp.stack(states)
    plane_flux = jnp.stack([jnp.stack(planes[0]), jnp.stack(planes[1])])
    return (state, plane_flux)
```

```python
import functools
import math

import jax
import jax.numpy as jnp
from jax import lax
from jax.experimental import pallas as pl
from jax.experimental.pallas import tpu as pltpu
from jax.sharding import PartitionSpec as P

F32 = jnp.float32
MESH = pl.DeviceIdType.MESH
TIME_STEP = 0.04
HALF_STEP = 0.5 * TIME_STEP
LANES = 128
INLET = (1.0, 0.5, 0.0, 0.0, 2.625)
INLET_U = 0.5
INLET_P = 1.0
INLET_SOUND = math.sqrt(1.4)


def derived(cells):
    density, m0, m1, m2, energy = cells
    inverse = 1.0 / density
    u0, u1, u2 = m0 * inverse, m1 * inverse, m2 * inverse
    pressure = 0.4 * (energy - 0.5 * (m0 * u0 + m1 * u1 + m2 * u2))
    sound = jnp.sqrt(1.4 * pressure * inverse)
    return (u0, u1, u2, pressure, sound)


def twice_flux(left, right, direction):
    cells_l, u_l, p_l, a_l = left
    cells_r, u_r, p_r, a_r = right
    speed = jnp.maximum(a_l, a_r)
    up, down = u_l + speed, u_r - speed
    out = [cells_l[j] * up + cells_r[j] * down for j in range(5)]
    out[1 + direction] = out[1 + direction] + (p_l + p_r)
    out[4] = out[4] + (p_l * u_l + p_r * u_r)
    return out


def along(cells, prims, direction):
    normal = prims[direction]
    return (cells, normal, prims[3], jnp.abs(normal) + prims[4])


def source(cells, force):
    return [
        None,
        cells[0] * force[0],
        cells[0] * force[1],
        cells[0] * force[2],
        cells[1] * force[0] + cells[2] * force[1] + cells[3] * force[2],
    ]


def advanced(cells, div, src):
    out = []
    for j in range(5):
        value = cells[j] - HALF_STEP * div[j]
        if src[j] is not None:
            value = value + TIME_STEP * src[j]
        out.append(value)
    return out


def kernel(
    sectors,
    bands,
    dens,
    vel,
    pres,
    forc,
    offs,
    wts,
    out,
    pf_out,
    U,
    W,
    FO,
    SS,
    SR,
    SP,
    TF,
    PS,
    PR0,
    PR1,
    PN,
    OB,
    PF,
    off_s,
    wts_s,
    in_sem,
    out_sem,
    ps_sem,
    pr_sem,
    ns_sem,
    nr_sem,
    hs_sem,
    hr_sem,
):
    row = lax.axis_index("row")
    circ = lax.axis_index("circ")
    span = lax.axis_index("span")
    cd = FO.shape[2]
    cycle = sectors * cd
    c_low, c_high = lax.rem(circ + sectors - 1, sectors), lax.rem(circ + 1, sectors)
    has_low, has_high = span > 0, span < bands - 1
    rotor = row == 0
    half = 1 - row

    barrier = pltpu.get_barrier_semaphore()
    for i in range(sectors):
        q = lax.rem(circ + sectors // 2 + i, sectors)
        pl.semaphore_signal(
            barrier, inc=1, device_id={"row": 1 - row, "circ": q}, device_id_type=MESH
        )
    for q in (c_low, c_high):
        pl.semaphore_signal(barrier, inc=1, device_id={"circ": q}, device_id_type=MESH)

    @pl.when(has_low)
    def _():
        pl.semaphore_signal(barrier, inc=1, device_id={"span": span - 1}, device_id_type=MESH)

    @pl.when(has_high)
    def _():
        pl.semaphore_signal(barrier, inc=1, device_id={"span": span + 1}, device_id_type=MESH)

    own = pl.ds(1, cd)
    PR = (PR0, PR1)
    loads = []

    def load(src, dst):
        copy = pltpu.make_async_copy(src, dst, in_sem.at[len(loads)])
        copy.start()
        loads.append(copy)

    for h in range(2):
        lanes = pl.ds(h * LANES, LANES)
        load(dens.at[0, :, :, lanes], U.at[0, 0, h, own])
        load(vel.at[0, :, :, :, lanes], U.at[0, pl.ds(1, 3), h, own])
        load(pres.at[0, :, :, lanes], U.at[0, 4, h, own])
    state_loads = len(loads)
    for h in range(2):
        load(forc.at[0, :, :, :, pl.ds(h * LANES, LANES)], FO.at[:, h])
    load(offs, off_s)
    load(wts, wts_s)
    for copy in loads[:state_loads]:
        copy.wait()

    lane = lax.broadcasted_iota(jnp.int32, (8, LANES), 1)
    sub = lax.broadcasted_iota(jnp.int32, (8, LANES), 0)
    block = lane // 16

    def conserve(c, _):
        for h in range(2):
            r = U[0, 0, h, c]
            v = [U[0, 1 + d, h, c] for d in range(3)]
            p = U[0, 4, h, c]
            for d in range(3):
                U[0, 1 + d, h, c] = r * v[d]
            U[0, 4, h, c] = p * 2.5 + 0.5 * r * (v[0] * v[0] + v[1] * v[1] + v[2] * v[2])
        return _

    lax.fori_loop(1, cd + 1, conserve, 0)

    def to_tile(line):
        tile = jnp.broadcast_to(line, (8, LANES))
        for bit in (4, 2, 1):
            tile = jnp.where((sub & bit) != 0, pltpu.roll(tile, LANES - 16 * bit, 1), tile)
        return tile

    def end_layers(block_of):
        ends, nexts = [], []
        for turned in (jnp.transpose(b) for b in block_of):
            ends.append(to_tile(jnp.where(rotor, turned[127:128], turned[0:1])))
            nexts.append(to_tile(jnp.where(rotor, turned[126:127], turned[1:2])))
        return ends, nexts

    def packed(tiles):
        out = tiles[0]
        for f in range(1, 5):
            out = jnp.where(block == f, pltpu.roll(tiles[f], 16 * f, 1), out)
        return jnp.where(block < 5, out, 0.0)

    def unpacked(tile, offset=0):
        return [pltpu.roll(tile, (offset - 16 * f) % LANES, 1) for f in range(5)]

    def plane_copies(par):
        copies = []
        for i in range(sectors):
            q = lax.rem(circ + sectors // 2 + i, sectors)
            copies.append(
                pltpu.make_async_remote_copy(
                    src_ref=PS.at[par],
                    dst_ref=PR[par].at[pl.ds(pl.multiple_of(circ * 8, 8), 8)],
                    send_sem=ps_sem.at[par, i],
                    recv_sem=pr_sem.at[par, circ],
                    device_id={"row": 1 - row, "circ": q},
                    device_id_type=MESH,
                )
            )
        return copies

    def plane_arrivals(par):
        return [
            pltpu.make_async_remote_copy(
                src_ref=PS.at[par],
                dst_ref=PR[par].at[pl.ds(q * 8, 8)],
                send_sem=ps_sem.at[par, q],
                recv_sem=pr_sem.at[par, q],
                device_id={"row": 1 - row},
                device_id_type=MESH,
            )
            for q in range(sectors)
        ]

    def to_neighbour(side, src, dst, send_sem, recv_sem):
        where = (
            {"circ": c_high},
            {"circ": c_low},
            {"span": span + 1},
            {"span": span - 1},
        )[side]
        return pltpu.make_async_remote_copy(
            src_ref=src,
            dst_ref=dst,
            send_sem=send_sem,
            recv_sem=recv_sem,
            device_id=where,
            device_id_type=MESH,
        )

    def near_plane(par, side):
        return to_neighbour(
            side, PS.at[par], PN.at[par, side], ns_sem.at[par, side], nr_sem.at[par, side]
        )

    def halo(par, side):
        if side < 2:
            src = U.at[par, :, :, cd if side == 0 else 1]
            dst = U.at[par, :, :, 0 if side == 0 else cd + 1]
        else:
            src, dst = SS.at[par, side - 2], SR.at[par, side - 2]
        return to_neighbour(side, src, dst, hs_sem.at[par, side], hr_sem.at[par, side])

    sends = (None, None, has_high, has_low)
    takes = (None, None, has_low, has_high)

    def guarded(condition, act):
        if condition is None:
            act()
        else:
            pl.when(condition)(act)

    def start_all(make, par):
        for side in range(4):
            guarded(sends[side], lambda side=side: make(par, side).start())

    def take_all(make, par):
        for side in range(4):
            guarded(takes[side], lambda side=side: make(par, side).wait_recv())

    def drain_all(make, par):
        for side in range(4):
            guarded(sends[side], lambda side=side: make(par, side).wait_send())

    def pack_span(par):
        for f in range(5):
            for h in range(2):
                cells = U[par, f, h, own]
                SS[par, 0, f, h] = cells[:, 15]
                SS[par, 1, f, h] = cells[:, 0]

    def mirror_span(par):
        def hub():
            for f in range(5):
                for h in range(2):
                    edge = SS[par, 1, f, h]
                    SR[par, 0, f, h] = -edge if f == 3 else edge

        def casing():
            for f in range(5):
                for h in range(2):
                    edge = SS[par, 0, f, h]
                    SR[par, 1, f, h] = -edge if f == 3 else edge

        pl.when(jnp.logical_not(has_low))(hub)
        pl.when(jnp.logical_not(has_high))(casing)

    def compact_base(par, ends, nexts, force):
        prims = derived(ends)
        near = [PN[par, k] for k in range(4)]
        flip = [-1.0 if f == 3 else 1.0 for f in range(5)]
        c_lo, c_hi = unpacked(near[0]), unpacked(near[1])
        s_lo = unpacked(near[2], -15)
        s_hi = unpacked(near[3], 15)
        below, above, left, right = [], [], [], []
        for f in range(5):
            below.append(jnp.where(sub == 0, c_lo[f][7:8], pltpu.roll(ends[f], 1, 0)))
            above.append(jnp.where(sub == 7, c_hi[f][0:1], pltpu.roll(ends[f], 7, 0)))
            low = jnp.where(has_low, s_lo[f], flip[f] * ends[f])
            left.append(jnp.where(lane == 0, low, pltpu.roll(ends[f], 1, 1)))
            high = jnp.where(has_high, s_hi[f], flip[f] * ends[f])
            right.append(jnp.where(lane == 15, high, pltpu.roll(ends[f], LANES - 1, 1)))

        def whole(cells, direction):
            return along(cells, derived(cells), direction)

        mid = [along(ends, prims, d) for d in range(3)]
        c_up = twice_flux(mid[1], whole(above, 1), 1)
        c_dn = twice_flux(whole(below, 1), mid[1], 1)
        s_up = twice_flux(mid[2], whole(right, 2), 2)
        s_dn = twice_flux(whole(left, 2), mid[2], 2)
        other = [jnp.where(rotor, b, a) for a, b in zip(ends, nexts)]
        inner = [jnp.where(rotor, a, b) for a, b in zip(ends, nexts)]
        axial = twice_flux(whole(other, 0), whole(inner, 0), 0)
        sign = jnp.where(rotor, 1.0, -1.0)
        div = [
            (c_up[j] - c_dn[j]) + (s_up[j] - s_dn[j]) - sign * axial[j] for j in range(5)
        ]
        return advanced(ends, div, source(ends, force))

    def compact_finish(par, ends, base):
        PR[par][pl.ds(cycle, 16)] = PR[par][pl.ds(0, 16)]
        turn = off_s[par]
        turn = jnp.where(rotor, turn, cycle - turn)
        start = lax.rem(circ * cd + turn - 1 + cycle, cycle)
        taps = [jnp.full((8, LANES), wts_s[par, k], F32) for k in range(4)]
        scale = 1.0 / ((taps[0] + taps[1]) + (taps[2] + taps[3]))
        ghost = jnp.zeros((8, LANES), F32)
        for k in range(4):
            ghost = ghost + (taps[k] * scale) * PR[par][pl.ds(start + k, 8), :]
        ghost = unpacked(ghost)
        left = [jnp.where(rotor, a, b) for a, b in zip(ends, ghost)]
        right = [jnp.where(rotor, b, a) for a, b in zip(ends, ghost)]
        plane = twice_flux(
            along(left, derived(left), 0), along(right, derived(right), 0), 0
        )
        for j in range(5):
            PF[par, j] = 0.5 * plane[j][:, :16]
        step = jnp.where(rotor, -HALF_STEP, HALF_STEP)
        return [base[j] + step * plane[j] for j in range(5)]

    def insert(par_tile, dest):
        turned = jnp.transpose(par_tile)
        here = lax.broadcasted_iota(jnp.int32, (16, LANES), 1) == jnp.where(rotor, 127, 0)
        for f in range(5):
            for c in range(cd):
                column = jnp.broadcast_to(turned[16 * f : 16 * f + 16, c : c + 1], (16, LANES))
                dest(f, c, here, column)

    def prim_rows(par, first, last):
        def one(c, _):
            for h in range(2):
                values = derived([U[par, f, h, c] for f in range(5)])
                for k in range(5):
                    W[k, h, c] = values[k]
            return _

        lax.fori_loop(first, last, one, 0)

    lane16 = lax.broadcasted_iota(jnp.int32, (16, LANES), 1)
    sub16 = lax.broadcasted_iota(jnp.int32, (16, LANES), 0)

    def span_edges(par):
        for h in range(2):
            low = [SR[par, 0, f, h] for f in range(5)]
            prims = derived(low)
            SP[0, h] = prims[2]
            SP[1, h] = prims[3]
            SP[2, h] = jnp.abs(prims[2]) + prims[4]
            high = [SR[par, 1, f, h] for f in range(5)]
            mine = [SS[par, 0, f, h] for f in range(5)]
            top = twice_flux(
                along(mine, derived(mine), 2), along(high, derived(high), 2), 2
            )
            for f in range(5):
                TF[f, h] = top[f]

    def bulk(par, store):
        def state_at(c):
            return [
                ([U[par, f, h, c] for f in range(5)], [W[k, h, c] for k in range(5)])
                for h in range(2)
            ]

        def c_faces(low, high):
            return tuple(
                tuple(
                    twice_flux(along(*low[h], 1), along(*high[h], 1), 1) for h in range(2)
                )
            )

        def one(c, lower):
            here = state_at(c + 1)
            upper = c_faces(here, state_at(c + 2))
            div = [[upper[h][j] - lower[h][j] for j in range(5)] for h in range(2)]

            full = [along(*here[h], 0) for h in range(2)]

            def before(pick, inlet):
                turned = [pltpu.roll(pick(full[h]), 1, 1) for h in range(2)]
                return (
                    jnp.where(lane16 == 0, inlet, turned[0]),
                    jnp.where(lane16 == 0, turned[0], turned[1]),
                )

            cells = [before(lambda s, f=f: s[0][f], INLET[f]) for f in range(5)]
            u = before(lambda s: s[1], INLET_U)
            p = before(lambda s: s[2], INLET_P)
            a = before(lambda s: s[3], INLET_U + INLET_SOUND)
            flux = [
                twice_flux(([x[h] for x in cells], u[h], p[h], a[h]), full[h], 0)
                for h in range(2)
            ]
            last = twice_flux(full[1], full[1], 0)
            for j in range(5):
                turned = [pltpu.roll(flux[h][j], LANES - 1, 1) for h in range(2)]
                div[0][j] += jnp.where(lane16 == 127, turned[1], turned[0]) - flux[0][j]
                div[1][j] += jnp.where(lane16 == 127, last[j], turned[1]) - flux[1][j]

            for h in range(2):
                full = along(*here[h], 2)

                def under(value, edge):
                    return jnp.where(sub16 == 0, edge, pltpu.roll(value, 1, 0))

                edge_row = pl.ds(c, 1)
                cells = [
                    under(full[0][f], SR[par, 0, f, h, edge_row, :]) for f in range(5)
                ]
                flux = twice_flux(
                    (
                        cells,
                        under(full[1], SP[0, h, edge_row, :]),
                        under(full[2], SP[1, h, edge_row, :]),
                        under(full[3], SP[2, h, edge_row, :]),
                    ),
                    full,
                    2,
                )
                for j in range(5):
                    above = jnp.where(
                        sub16 == 15, TF[j, h, edge_row, :], pltpu.roll(flux[j], 15, 0)
                    )
                    div[h][j] += above - flux[j]
                force = [FO[d, h, c] for d in range(3)]
                new = advanced(here[h][0], div[h], source(here[h][0], force))
                for j in range(5):
                    store(j, h, c, new[j])
            return upper

        lax.fori_loop(0, cd, one, c_faces(state_at(0), state_at(1)))

    def blocks_of(ref):
        return [ref(f).reshape(cd * 16, LANES) for f in range(5)]

    ends, nexts = end_layers(blocks_of(lambda f: U[0, f, half, own]))
    PS[0] = packed(ends)
    pack_span(0)
    peers = sectors + 2 + has_low.astype(jnp.int32) + has_high.astype(jnp.int32)
    pl.semaphore_wait(barrier, peers)
    sent = plane_copies(0)
    for copy in sent:
        copy.start()
    start_all(near_plane, 0)
    start_all(halo, 0)
    mirror_span(0)
    for copy in loads[state_loads:]:
        copy.wait()
    force, _ = end_layers([FO[d, half].reshape(cd * 16, LANES) for d in range(3)])
    prim_rows(0, 1, cd + 1)
    take_all(near_plane, 0)
    base = compact_base(0, ends, nexts, force)
    take_all(halo, 0)
    prim_rows(0, 0, 1)
    prim_rows(0, cd + 1, cd + 2)
    span_edges(0)

    def keep(j, h, c, value):
        U[1, j, h, c + 1] = value

    bulk(0, keep)
    for copy in plane_arrivals(0):
        copy.wait_recv()
    ends = compact_finish(0, ends, base)
    tile = packed(ends)
    PS[1] = tile
    sent_next = plane_copies(1)
    for copy in sent_next:
        copy.start()
    start_all(near_plane, 1)

    def into_state(f, c, here, column):
        U[1, f, half, c + 1] = jnp.where(here, column, U[1, f, half, c + 1])

    insert(tile, into_state)
    pack_span(1)
    start_all(halo, 1)
    mirror_span(1)

    _, nexts = end_layers(blocks_of(lambda f: U[1, f, half, own]))
    prim_rows(1, 1, cd + 1)
    take_all(near_plane, 1)
    base = compact_base(1, ends, nexts, force)
    take_all(halo, 1)
    prim_rows(1, 0, 1)
    prim_rows(1, cd + 1, cd + 2)
    span_edges(1)

    def emit(j, h, c, value):
        OB[j, h, c] = value

    bulk(1, emit)

    def store_half(h, lane_start, sem):
        return pltpu.make_async_copy(
            OB.at[:, h], out.at[0, :, :, :, pl.ds(lane_start, LANES)], sem
        )

    for copy in plane_arrivals(1):
        copy.wait_recv()
    ends = compact_finish(1, ends, base)

    def into_out(f, c, here, column):
        OB[f, half, c] = jnp.where(here, column, OB[f, half, c])

    insert(packed(ends), into_out)
    writes = [store_half(h, h * LANES, out_sem.at[h]) for h in range(2)]
    writes.append(pltpu.make_async_copy(PF, pf_out.at[0], out_sem.at[2]))
    for copy in writes:
        copy.start()
    for copies in (sent, sent_next):
        for copy in copies:
            copy.wait_send()
    for par in range(2):
        drain_all(near_plane, par)
        drain_all(halo, par)
    for copy in writes:
        copy.wait()


def solution(mesh):
    sectors = mesh.shape["circ"]
    bands = mesh.shape["span"]

    def body(density, velocity, pressure, blade_force, offsets, weights):
        _, cd, sd, axial = density.shape
        vmem, dma = pltpu.VMEM, pltpu.SemaphoreType.DMA
        any_space = pl.BlockSpec(memory_space=pl.ANY)
        return pl.pallas_call(
            functools.partial(kernel, sectors, bands),
            out_shape=(
                jax.ShapeDtypeStruct((1, 5, cd, sd, axial), F32),
                jax.ShapeDtypeStruct((1, 2, 5, cd, sd), F32),
            ),
            in_specs=[any_space] * 6,
            out_specs=(any_space, any_space),
            scratch_shapes=[
                vmem((2, 5, 2, cd + 2, sd, LANES), F32),
                vmem((5, 2, cd + 2, sd, LANES), F32),
                vmem((3, 2, cd, sd, LANES), F32),
                vmem((2, 2, 5, 2, cd, LANES), F32),
                vmem((2, 2, 5, 2, cd, LANES), F32),
                vmem((3, 2, cd, LANES), F32),
                vmem((5, 2, cd, LANES), F32),
                vmem((2, 8, LANES), F32),
                vmem(((sectors + 2) * 8, LANES), F32),
                vmem(((sectors + 2) * 8, LANES), F32),
                vmem((2, 4, 8, LANES), F32),
                vmem((5, 2, cd, sd, LANES), F32),
                vmem((2, 5, cd, sd), F32),
                pltpu.SMEM((2,), jnp.int32),
                pltpu.SMEM((2, 4), F32),
                dma((10,)),
                dma((3,)),
                dma((2, sectors)),
                dma((2, sectors)),
                dma((2, 4)),
                dma((2, 4)),
                dma((2, 4)),
                dma((2, 4)),
            ],
            compiler_params=pltpu.CompilerParams(collective_id=0, has_side_effects=True),
        )(density, velocity, pressure, blade_force, offsets, weights)

    placed = (
        P("row", "circ", "span", None),
        P("row", None, "circ", "span", None),
        P("row", "circ", "span", None),
        P("row", None, "circ", "span", None),
        P(),
        P(),
    )
    return jax.shard_map(
        body,
        mesh=mesh,
        in_specs=placed,
        out_specs=(P("row", None, "circ", "span", None), P("row", None, None, "circ", "span")),
        check_vma=False,
    )
```

```python
import functools
import math

import jax
import jax.numpy as jnp
from jax import lax
from jax.experimental import pallas as pl
from jax.experimental.pallas import tpu as pltpu
from jax.sharding import PartitionSpec as P

F32 = jnp.float32
MESH = pl.DeviceIdType.MESH
TIME_STEP = 0.04
HALF_STEP = 0.5 * TIME_STEP
LANES = 128
INLET = (1.0, 0.5, 0.0, 0.0, 2.625)
INLET_U = 0.5
INLET_P = 1.0
INLET_SOUND = math.sqrt(1.4)


def derived(cells):
    density, m0, m1, m2, energy = cells
    inverse = 1.0 / density
    u0, u1, u2 = m0 * inverse, m1 * inverse, m2 * inverse
    pressure = 0.4 * (energy - 0.5 * (m0 * u0 + m1 * u1 + m2 * u2))
    sound = jnp.sqrt(1.4 * pressure * inverse)
    return (u0, u1, u2, pressure, sound)


def twice_flux(left, right, direction):
    cells_l, u_l, p_l, a_l = left
    cells_r, u_r, p_r, a_r = right
    speed = jnp.maximum(a_l, a_r)
    up, down = u_l + speed, u_r - speed
    out = [cells_l[j] * up + cells_r[j] * down for j in range(5)]
    out[1 + direction] = out[1 + direction] + (p_l + p_r)
    out[4] = out[4] + (p_l * u_l + p_r * u_r)
    return out


def along(cells, prims, direction):
    normal = prims[direction]
    return (cells, normal, prims[3], jnp.abs(normal) + prims[4])


def source(cells, force):
    return [
        None,
        cells[0] * force[0],
        cells[0] * force[1],
        cells[0] * force[2],
        cells[1] * force[0] + cells[2] * force[1] + cells[3] * force[2],
    ]


def advanced(cells, div, src):
    out = []
    for j in range(5):
        value = cells[j] - HALF_STEP * div[j]
        if src[j] is not None:
            value = value + TIME_STEP * src[j]
        out.append(value)
    return out


def kernel(
    sectors,
    bands,
    dens,
    vel,
    pres,
    forc,
    offs,
    wts,
    OB,
    PF,
    U,
    W,
    FO,
    SS,
    SR,
    PS,
    PR0,
    PR1,
    PN,
    off_s,
    wts_s,
    in_sem,
    ps_sem,
    pr_sem,
    ns_sem,
    nr_sem,
    hs_sem,
    hr_sem,
):
    row = lax.axis_index("row")
    circ = lax.axis_index("circ")
    span = lax.axis_index("span")
    cd = FO.shape[2]
    cycle = sectors * cd
    c_low, c_high = lax.rem(circ + sectors - 1, sectors), lax.rem(circ + 1, sectors)
    has_low, has_high = span > 0, span < bands - 1
    rotor = row == 0
    half = 1 - row

    barrier = pltpu.get_barrier_semaphore()
    for i in range(sectors):
        q = lax.rem(circ + sectors // 2 + i, sectors)
        pl.semaphore_signal(
            barrier, inc=1, device_id={"row": 1 - row, "circ": q}, device_id_type=MESH
        )
    for q in (c_low, c_high):
        pl.semaphore_signal(barrier, inc=1, device_id={"circ": q}, device_id_type=MESH)

    @pl.when(has_low)
    def _():
        pl.semaphore_signal(barrier, inc=1, device_id={"span": span - 1}, device_id_type=MESH)

    @pl.when(has_high)
    def _():
        pl.semaphore_signal(barrier, inc=1, device_id={"span": span + 1}, device_id_type=MESH)

    own = pl.ds(1, cd)
    PR = (PR0, PR1)
    loads = []

    def load(src, dst):
        copy = pltpu.make_async_copy(src, dst, in_sem.at[len(loads)])
        copy.start()
        loads.append(copy)

    for h in (half, row):
        lanes = pl.ds(pl.multiple_of(h * LANES, LANES), LANES)
        load(dens.at[0, :, :, lanes], U.at[0, 0, h, own])
        load(vel.at[0, :, :, :, lanes], U.at[0, pl.ds(1, 3), h, own])
        load(pres.at[0, :, :, lanes], U.at[0, 4, h, own])
    state_loads = len(loads)
    for h in range(2):
        load(forc.at[0, :, :, :, pl.ds(h * LANES, LANES)], FO.at[:, h])
    load(offs, off_s)
    load(wts, wts_s)

    lane = lax.broadcasted_iota(jnp.int32, (8, LANES), 1)
    sub = lax.broadcasted_iota(jnp.int32, (8, LANES), 0)
    block = lane // 16

    def conserve(c, _):
        for h in range(2):
            r = U[0, 0, h, c]
            v = [U[0, 1 + d, h, c] for d in range(3)]
            p = U[0, 4, h, c]
            for d in range(3):
                U[0, 1 + d, h, c] = r * v[d]
            U[0, 4, h, c] = p * 2.5 + 0.5 * r * (v[0] * v[0] + v[1] * v[1] + v[2] * v[2])
        return _

    def to_tile(line):
        tile = jnp.broadcast_to(line, (8, LANES))
        for bit in (4, 2, 1):
            tile = jnp.where((sub & bit) != 0, pltpu.roll(tile, LANES - 16 * bit, 1), tile)
        return tile

    def end_layers(block_of):
        ends, nexts = [], []
        for turned in (jnp.transpose(b) for b in block_of):
            ends.append(to_tile(jnp.where(rotor, turned[127:128], turned[0:1])))
            nexts.append(to_tile(jnp.where(rotor, turned[126:127], turned[1:2])))
        return ends, nexts

    def packed(tiles):
        out = tiles[0]
        for f in range(1, 5):
            out = jnp.where(block == f, pltpu.roll(tiles[f], 16 * f, 1), out)
        return jnp.where(block < 5, out, 0.0)

    def unpacked(tile, offset=0):
        return [pltpu.roll(tile, (offset - 16 * f) % LANES, 1) for f in range(5)]

    def plane_copies(par):
        copies = []
        for i in range(sectors):
            q = lax.rem(circ + sectors // 2 + i, sectors)
            copies.append(
                pltpu.make_async_remote_copy(
                    src_ref=PS.at[par],
                    dst_ref=PR[par].at[pl.ds(pl.multiple_of(circ * 8, 8), 8)],
                    send_sem=ps_sem.at[par, i],
                    recv_sem=pr_sem.at[par, circ],
                    device_id={"row": 1 - row, "circ": q},
                    device_id_type=MESH,
                )
            )
        return copies

    def plane_arrivals(par):
        return [
            pltpu.make_async_remote_copy(
                src_ref=PS.at[par],
                dst_ref=PR[par].at[pl.ds(q * 8, 8)],
                send_sem=ps_sem.at[par, q],
                recv_sem=pr_sem.at[par, q],
                device_id={"row": 1 - row},
                device_id_type=MESH,
            )
            for q in range(sectors)
        ]

    def to_neighbour(side, src, dst, send_sem, recv_sem):
        where = (
            {"circ": c_high},
            {"circ": c_low},
            {"span": span + 1},
            {"span": span - 1},
        )[side]
        return pltpu.make_async_remote_copy(
            src_ref=src,
            dst_ref=dst,
            send_sem=send_sem,
            recv_sem=recv_sem,
            device_id=where,
            device_id_type=MESH,
        )

    def near_plane(par, side):
        return to_neighbour(
            side, PS.at[par], PN.at[par, side], ns_sem.at[par, side], nr_sem.at[par, side]
        )

    def halo(par, side):
        if side < 2:
            src = U.at[par, :, :, cd if side == 0 else 1]
            dst = U.at[par, :, :, 0 if side == 0 else cd + 1]
        else:
            src, dst = SS.at[par, side - 2], SR.at[par, side - 2]
        return to_neighbour(side, src, dst, hs_sem.at[par, side], hr_sem.at[par, side])

    sends = (None, None, has_high, has_low)
    takes = (None, None, has_low, has_high)

    def guarded(condition, act):
        if condition is None:
            act()
        else:
            pl.when(condition)(act)

    def start_all(make, par):
        for side in range(4):
            guarded(sends[side], lambda side=side: make(par, side).start())

    def take_all(make, par):
        for side in range(4):
            guarded(takes[side], lambda side=side: make(par, side).wait_recv())

    def drain_all(make, par):
        for side in range(4):
            guarded(sends[side], lambda side=side: make(par, side).wait_send())

    def pack_span(par):
        for f in range(5):
            for h in range(2):
                cells = U[par, f, h, own]
                SS[par, 0, f, h] = cells[:, 15]
                SS[par, 1, f, h] = cells[:, 0]

    def mirror_span(par):
        def hub():
            for f in range(5):
                for h in range(2):
                    edge = SS[par, 1, f, h]
                    SR[par, 0, f, h] = -edge if f == 3 else edge

        def casing():
            for f in range(5):
                for h in range(2):
                    edge = SS[par, 0, f, h]
                    SR[par, 1, f, h] = -edge if f == 3 else edge

        pl.when(jnp.logical_not(has_low))(hub)
        pl.when(jnp.logical_not(has_high))(casing)

    def compact_base(par, ends, nexts, force):
        prims = derived(ends)
        near = [PN[par, k] for k in range(4)]
        flip = [-1.0 if f == 3 else 1.0 for f in range(5)]
        c_lo, c_hi = unpacked(near[0]), unpacked(near[1])
        s_lo = unpacked(near[2], -15)
        s_hi = unpacked(near[3], 15)
        below, above, left, right = [], [], [], []
        for f in range(5):
            below.append(jnp.where(sub == 0, c_lo[f][7:8], pltpu.roll(ends[f], 1, 0)))
            above.append(jnp.where(sub == 7, c_hi[f][0:1], pltpu.roll(ends[f], 7, 0)))
            low = jnp.where(has_low, s_lo[f], flip[f] * ends[f])
            left.append(jnp.where(lane == 0, low, pltpu.roll(ends[f], 1, 1)))
            high = jnp.where(has_high, s_hi[f], flip[f] * ends[f])
            right.append(jnp.where(lane == 15, high, pltpu.roll(ends[f], LANES - 1, 1)))

        def whole(cells, direction):
            return along(cells, derived(cells), direction)

        mid = [along(ends, prims, d) for d in range(3)]
        c_up = twice_flux(mid[1], whole(above, 1), 1)
        c_dn = twice_flux(whole(below, 1), mid[1], 1)
        s_up = twice_flux(mid[2], whole(right, 2), 2)
        s_dn = twice_flux(whole(left, 2), mid[2], 2)
        other = [jnp.where(rotor, b, a) for a, b in zip(ends, nexts)]
        inner = [jnp.where(rotor, a, b) for a, b in zip(ends, nexts)]
        axial = twice_flux(whole(other, 0), whole(inner, 0), 0)
        sign = jnp.where(rotor, 1.0, -1.0)
        div = [
            (c_up[j] - c_dn[j]) + (s_up[j] - s_dn[j]) - sign * axial[j] for j in range(5)
        ]
        return advanced(ends, div, source(ends, force))

    def compact_finish(par, ends, base):
        PR[par][pl.ds(cycle, 16)] = PR[par][pl.ds(0, 16)]
        turn = off_s[par]
        turn = jnp.where(rotor, turn, cycle - turn)
        start = lax.rem(circ * cd + turn - 1 + cycle, cycle)
        taps = [jnp.full((8, LANES), wts_s[par, k], F32) for k in range(4)]
        scale = 1.0 / ((taps[0] + taps[1]) + (taps[2] + taps[3]))
        ghost = jnp.zeros((8, LANES), F32)
        for k in range(4):
            ghost = ghost + (taps[k] * scale) * PR[par][pl.ds(start + k, 8), :]
        ghost = unpacked(ghost)
        left = [jnp.where(rotor, a, b) for a, b in zip(ends, ghost)]
        right = [jnp.where(rotor, b, a) for a, b in zip(ends, ghost)]
        plane = twice_flux(
            along(left, derived(left), 0), along(right, derived(right), 0), 0
        )
        for j in range(5):
            PF[0, par, j] = 0.5 * plane[j][:, :16]
        step = jnp.where(rotor, -HALF_STEP, HALF_STEP)
        return [base[j] + step * plane[j] for j in range(5)]

    def insert(par_tile, dest):
        turned = jnp.transpose(par_tile)
        here = lax.broadcasted_iota(jnp.int32, (16, LANES), 1) == jnp.where(rotor, 127, 0)
        for f in range(5):
            for c in range(cd):
                column = jnp.broadcast_to(turned[16 * f : 16 * f + 16, c : c + 1], (16, LANES))
                dest(f, c, here, column)

    def prim_rows(par, first, last):
        def one(c, _):
            for h in range(2):
                values = derived([U[par, f, h, c] for f in range(5)])
                for k in range(5):
                    W[k, h, c] = values[k]
            return _

        lax.fori_loop(first, last, one, 0)

    lane16 = lax.broadcasted_iota(jnp.int32, (16, LANES), 1)
    sub16 = lax.broadcasted_iota(jnp.int32, (16, LANES), 0)

    def bulk(par, store):
        def state_at(c):
            return [
                ([U[par, f, h, c] for f in range(5)], [W[k, h, c] for k in range(5)])
                for h in range(2)
            ]

        def one(c, lower, last_row):
            here = state_at(c + 1)
            if last_row:
                upper = None
                div = [[-lower[h][j] for j in range(5)] for h in range(2)]
            else:
                there = state_at(c + 2)
                upper = tuple(
                    tuple(twice_flux(along(*here[h], 1), along(*there[h], 1), 1))
                    for h in range(2)
                )
                div = [[upper[h][j] - lower[h][j] for j in range(5)] for h in range(2)]

            full = [along(*here[h], 0) for h in range(2)]

            def before(pick, inlet):
                turned = [pltpu.roll(pick(full[h]), 1, 1) for h in range(2)]
                return (
                    jnp.where(lane16 == 0, inlet, turned[0]),
                    jnp.where(lane16 == 0, turned[0], turned[1]),
                )

            cells = [before(lambda s, f=f: s[0][f], INLET[f]) for f in range(5)]
            u = before(lambda s: s[1], INLET_U)
            p = before(lambda s: s[2], INLET_P)
            a = before(lambda s: s[3], INLET_U + INLET_SOUND)
            flux = [
                twice_flux(([x[h] for x in cells], u[h], p[h], a[h]), full[h], 0)
                for h in range(2)
            ]
            last = twice_flux(full[1], full[1], 0)
            for j in range(5):
                turned = [pltpu.roll(flux[h][j], LANES - 1, 1) for h in range(2)]
                div[0][j] += jnp.where(lane16 == 127, turned[1], turned[0]) - flux[0][j]
                div[1][j] += jnp.where(lane16 == 127, last[j], turned[1]) - flux[1][j]

            for h in range(2):
                full = along(*here[h], 2)
                flux = twice_flux(
                    (
                        [pltpu.roll(full[0][f], 1, 0) for f in range(5)],
                        pltpu.roll(full[1], 1, 0),
                        pltpu.roll(full[2], 1, 0),
                        pltpu.roll(full[3], 1, 0),
                    ),
                    full,
                    2,
                )
                for j in range(5):
                    inside = jnp.where(sub16 == 0, 0.0, flux[j])
                    div[h][j] += pltpu.roll(inside, 15, 0) - inside
                force = [FO[d, h, c] for d in range(3)]
                new = advanced(here[h][0], div[h], source(here[h][0], force))
                for j in range(5):
                    store(j, h, c, new[j])
            return upper

        none = jnp.zeros((16, LANES), F32)
        start = tuple(tuple(none for _ in range(5)) for _ in range(2))
        final = lax.fori_loop(0, cd - 1, lambda c, lower: one(c, lower, False), start)
        one(cd - 1, final, True)

    def edges(par, shift):
        def flux_of(low, high, direction):
            return twice_flux(
                along(low, derived(low), direction),
                along(high, derived(high), direction),
                direction,
            )

        for h in range(2):
            rows = [[U[par, f, h, c] for f in range(5)] for c in (0, 1, cd, cd + 1)]
            low = flux_of(rows[0], rows[1], 1)
            high = flux_of(rows[2], rows[3], 1)
            for j in range(5):
                shift(j, h, 0, pl.ds(0, 16), HALF_STEP * low[j])
                shift(j, h, cd - 1, pl.ds(0, 16), -HALF_STEP * high[j])
            bottom, top = ([SS[par, k, f, h] for f in range(5)] for k in (1, 0))
            below, above = ([SR[par, k, f, h] for f in range(5)] for k in (0, 1))
            low = flux_of(below, bottom, 2)
            high = flux_of(top, above, 2)
            for j in range(5):
                shift(j, h, pl.ds(0, cd), 0, HALF_STEP * low[j])
                shift(j, h, pl.ds(0, cd), 15, -HALF_STEP * high[j])

    def blocks_of(ref):
        return [ref(f).reshape(cd * 16, LANES) for f in range(5)]

    for copy in loads[:3]:
        copy.wait()
    (ends, nexts) = end_layers(blocks_of(lambda f: U[0, f, half, own]))

    def conserved(raw):
        r, v0, v1, v2, p = raw
        return [r, r * v0, r * v1, r * v2, p * 2.5 + 0.5 * r * (v0 * v0 + v1 * v1 + v2 * v2)]

    ends, nexts = conserved(ends), conserved(nexts)
    PS[0] = packed(ends)
    for copy in loads[3:state_loads]:
        copy.wait()
    lax.fori_loop(1, cd + 1, conserve, 0)
    pack_span(0)
    peers = sectors + 2 + has_low.astype(jnp.int32) + has_high.astype(jnp.int32)
    pl.semaphore_wait(barrier, peers)
    sent = plane_copies(0)
    for copy in sent:
        copy.start()
    start_all(near_plane, 0)
    start_all(halo, 0)
    mirror_span(0)
    for copy in loads[state_loads:]:
        copy.wait()
    force, _ = end_layers([FO[d, half].reshape(cd * 16, LANES) for d in range(3)])
    prim_rows(0, 1, cd + 1)

    def keep(j, h, c, value):
        U[1, j, h, c + 1] = value

    bulk(0, keep)
    take_all(near_plane, 0)
    base = compact_base(0, ends, nexts, force)
    for copy in plane_arrivals(0):
        copy.wait_recv()
    ends = compact_finish(0, ends, base)
    tile = packed(ends)
    PS[1] = tile
    sent_next = plane_copies(1)
    for copy in sent_next:
        copy.start()
    start_all(near_plane, 1)
    take_all(halo, 0)

    def shift_state(j, h, c, s, value):
        c = pl.ds(1, cd) if isinstance(c, pl.Slice) else c + 1
        U[1, j, h, c, s] = U[1, j, h, c, s] + value

    edges(0, shift_state)

    def into_state(f, c, here, column):
        U[1, f, half, c + 1] = jnp.where(here, column, U[1, f, half, c + 1])

    insert(tile, into_state)
    pack_span(1)
    start_all(halo, 1)
    mirror_span(1)

    _, nexts = end_layers(blocks_of(lambda f: U[1, f, half, own]))
    prim_rows(1, 1, cd + 1)

    def emit(j, h, c, value):
        OB[0, j, c, :, h * LANES : (h + 1) * LANES] = value

    bulk(1, emit)
    take_all(near_plane, 1)
    base = compact_base(1, ends, nexts, force)
    take_all(halo, 1)

    def shift_out(j, h, c, s, value):
        lanes = pl.ds(h * LANES, LANES)
        OB[0, j, c, s, lanes] = OB[0, j, c, s, lanes] + value

    edges(1, shift_out)
    for copy in plane_arrivals(1):
        copy.wait_recv()
    ends = compact_finish(1, ends, base)

    def into_out(f, c, here, column):
        lanes = pl.ds(pl.multiple_of(half * LANES, LANES), LANES)
        OB[0, f, c, :, lanes] = jnp.where(here, column, OB[0, f, c, :, lanes])

    insert(packed(ends), into_out)
    for copies in (sent, sent_next):
        for copy in copies:
            copy.wait_send()
    for par in range(2):
        drain_all(near_plane, par)
        drain_all(halo, par)


def write_out(state, plane, out, plane_out, sems):
    writes = [
        pltpu.make_async_copy(state, out, sems.at[0]),
        pltpu.make_async_copy(plane, plane_out, sems.at[1]),
    ]
    for copy in writes:
        copy.start()
    for copy in writes:
        copy.wait()


def solution(mesh):
    sectors = mesh.shape["circ"]
    bands = mesh.shape["span"]

    def body(density, velocity, pressure, blade_force, offsets, weights):
        _, cd, sd, axial = density.shape
        vmem, dma = pltpu.VMEM, pltpu.SemaphoreType.DMA
        any_space = pl.BlockSpec(memory_space=pl.ANY)
        in_vmem = pl.BlockSpec(memory_space=pltpu.VMEM)
        results = pl.pallas_call(
            functools.partial(kernel, sectors, bands),
            out_shape=(
                vmem((1, 5, cd, sd, axial), F32),
                vmem((1, 2, 5, cd, sd), F32),
            ),
            in_specs=[any_space] * 6,
            out_specs=(in_vmem, in_vmem),
            scratch_shapes=[
                vmem((2, 5, 2, cd + 2, sd, LANES), F32),
                vmem((5, 2, cd + 2, sd, LANES), F32),
                vmem((3, 2, cd, sd, LANES), F32),
                vmem((2, 2, 5, 2, cd, LANES), F32),
                vmem((2, 2, 5, 2, cd, LANES), F32),
                vmem((2, 8, LANES), F32),
                vmem(((sectors + 2) * 8, LANES), F32),
                vmem(((sectors + 2) * 8, LANES), F32),
                vmem((2, 4, 8, LANES), F32),
                pltpu.SMEM((2,), jnp.int32),
                pltpu.SMEM((2, 4), F32),
                dma((10,)),
                dma((2, sectors)),
                dma((2, sectors)),
                dma((2, 4)),
                dma((2, 4)),
                dma((2, 4)),
                dma((2, 4)),
            ],
            compiler_params=pltpu.CompilerParams(collective_id=0, has_side_effects=True),
        )(density, velocity, pressure, blade_force, offsets, weights)
        results = [pltpu.with_memory_space_constraint(x, pltpu.VMEM) for x in results]
        return pl.pallas_call(
            write_out,
            out_shape=(
                jax.ShapeDtypeStruct((1, 5, cd, sd, axial), F32),
                jax.ShapeDtypeStruct((1, 2, 5, cd, sd), F32),
            ),
            in_specs=[in_vmem, in_vmem],
            out_specs=(any_space, any_space),
            scratch_shapes=[dma((2,))],
        )(*results)

    placed = (
        P("row", "circ", "span", None),
        P("row", None, "circ", "span", None),
        P("row", "circ", "span", None),
        P("row", None, "circ", "span", None),
        P(),
        P(),
    )
    return jax.shard_map(
        body,
        mesh=mesh,
        in_specs=placed,
        out_specs=(P("row", None, "circ", "span", None), P("row", None, None, "circ", "span")),
        check_vma=False,
    )
```

```python
import functools
import math

import jax
import jax.numpy as jnp
from jax import lax
from jax.experimental import pallas as pl
from jax.experimental.pallas import tpu as pltpu
from jax.sharding import PartitionSpec as P

F32 = jnp.float32
MESH = pl.DeviceIdType.MESH
TIME_STEP = 0.04
HALF_STEP = 0.5 * TIME_STEP
LANES = 128
INLET = (1.0, 0.5, 0.0, 0.0, 2.625)
INLET_U = 0.5
INLET_P = 1.0
INLET_SOUND = math.sqrt(1.4)


def derived(cells):
    density, m0, m1, m2, energy = cells
    inverse = 1.0 / density
    u0, u1, u2 = m0 * inverse, m1 * inverse, m2 * inverse
    pressure = 0.4 * (energy - 0.5 * (m0 * u0 + m1 * u1 + m2 * u2))
    sound = jnp.sqrt(1.4 * pressure * inverse)
    return (u0, u1, u2, pressure, sound)


def twice_flux(left, right, direction):
    cells_l, u_l, p_l, a_l = left
    cells_r, u_r, p_r, a_r = right
    speed = jnp.maximum(a_l, a_r)
    up, down = u_l + speed, u_r - speed
    out = [cells_l[j] * up + cells_r[j] * down for j in range(5)]
    out[1 + direction] = out[1 + direction] + (p_l + p_r)
    out[4] = out[4] + (p_l * u_l + p_r * u_r)
    return out


def along(cells, prims, direction):
    normal = prims[direction]
    return (cells, normal, prims[3], jnp.abs(normal) + prims[4])


def source(cells, force):
    return [
        None,
        cells[0] * force[0],
        cells[0] * force[1],
        cells[0] * force[2],
        cells[1] * force[0] + cells[2] * force[1] + cells[3] * force[2],
    ]


def advanced(cells, div, src):
    out = []
    for j in range(5):
        value = cells[j] - HALF_STEP * div[j]
        if src[j] is not None:
            value = value + TIME_STEP * src[j]
        out.append(value)
    return out


def kernel(
    sectors,
    bands,
    dens,
    vel,
    pres,
    forc,
    offs,
    wts,
    OB,
    PF,
    U,
    W,
    FO,
    SS,
    SR,
    SC,
    PS,
    PR0,
    PR1,
    PN,
    off_s,
    wts_s,
    in_sem,
    ps_sem,
    pr_sem,
    ns_sem,
    nr_sem,
    hs_sem,
    hr_sem,
):
    row = lax.axis_index("row")
    circ = lax.axis_index("circ")
    span = lax.axis_index("span")
    cd = FO.shape[2]
    cycle = sectors * cd
    c_low, c_high = lax.rem(circ + sectors - 1, sectors), lax.rem(circ + 1, sectors)
    has_low, has_high = span > 0, span < bands - 1
    rotor = row == 0
    half = 1 - row

    own = pl.ds(1, cd)
    PR = (PR0, PR1)

    def load_half(h, sem):
        lanes = pl.ds(pl.multiple_of(h * LANES, LANES), LANES)
        for src, dst in (
            (dens.at[0, :, :, lanes], U.at[0, 0, h, own]),
            (vel.at[0, :, :, :, lanes], U.at[0, pl.ds(1, 3), h, own]),
            (pres.at[0, :, :, lanes], U.at[0, 4, h, own]),
        ):
            pltpu.make_async_copy(src, dst, in_sem.at[sem]).start()

    def loaded(ref, sem):
        pltpu.make_async_copy(ref, ref, in_sem.at[sem]).wait()

    load_half(half, 0)
    barrier = pltpu.get_barrier_semaphore()
    for i in range(sectors):
        q = lax.rem(circ + sectors // 2 + i, sectors)
        pl.semaphore_signal(
            barrier, inc=1, device_id={"row": 1 - row, "circ": q}, device_id_type=MESH
        )
    for q in (c_low, c_high):
        pl.semaphore_signal(barrier, inc=1, device_id={"circ": q}, device_id_type=MESH)

    @pl.when(has_low)
    def _():
        pl.semaphore_signal(barrier, inc=1, device_id={"span": span - 1}, device_id_type=MESH)

    @pl.when(has_high)
    def _():
        pl.semaphore_signal(barrier, inc=1, device_id={"span": span + 1}, device_id_type=MESH)

    load_half(row, 1)
    for h in range(2):
        lanes = pl.ds(h * LANES, LANES)
        pltpu.make_async_copy(forc.at[0, :, :, :, lanes], FO.at[:, h], in_sem.at[2]).start()
    load_offsets = pltpu.make_async_copy(offs, off_s, in_sem.at[3])
    load_weights = pltpu.make_async_copy(wts, wts_s, in_sem.at[4])
    load_offsets.start()
    load_weights.start()

    lane = lax.broadcasted_iota(jnp.int32, (5, LANES), 1)
    sub8 = lax.broadcasted_iota(jnp.int32, (8, LANES), 0)

    def conserve(c, _):
        for h in range(2):
            r = U[0, 0, h, c]
            v = [U[0, 1 + d, h, c] for d in range(3)]
            p = U[0, 4, h, c]
            for d in range(3):
                U[0, 1 + d, h, c] = r * v[d]
            U[0, 4, h, c] = p * 2.5 + 0.5 * r * (v[0] * v[0] + v[1] * v[1] + v[2] * v[2])
        return _

    def to_tile(line):
        tile = jnp.broadcast_to(line, (8, LANES))
        for bit in (4, 2, 1):
            tile = jnp.where((sub8 & bit) != 0, pltpu.roll(tile, LANES - 16 * bit, 1), tile)
        return tile

    def end_layers(block_of):
        ends, nexts = [], []
        for turned in (jnp.transpose(b) for b in block_of):
            ends.append(jnp.where(rotor, turned[127:128], turned[0:1]))
            nexts.append(jnp.where(rotor, turned[126:127], turned[1:2]))
        return ends, nexts

    def put_lines(par, lines):
        for f in range(5):
            PS[par, f : f + 1] = lines[f]

    def lines_of(stack):
        return [stack[f : f + 1] for f in range(5)]

    def plane_copies(par):
        copies = []
        for i in range(sectors):
            q = lax.rem(circ + sectors // 2 + i, sectors)
            copies.append(
                pltpu.make_async_remote_copy(
                    src_ref=PS.at[par],
                    dst_ref=PR[par].at[circ],
                    send_sem=ps_sem.at[par],
                    recv_sem=pr_sem.at[par],
                    device_id={"row": 1 - row, "circ": q},
                    device_id_type=MESH,
                )
            )
        return copies

    def all_planes(par):
        return pltpu.make_async_remote_copy(
            src_ref=PR[par],
            dst_ref=PR[par],
            send_sem=ps_sem.at[par],
            recv_sem=pr_sem.at[par],
            device_id={"row": 1 - row},
            device_id_type=MESH,
        )

    def to_neighbour(side, src, dst, send_sem, recv_sem):
        where = (
            {"circ": c_high},
            {"circ": c_low},
            {"span": span + 1},
            {"span": span - 1},
        )[side]
        return pltpu.make_async_remote_copy(
            src_ref=src,
            dst_ref=dst,
            send_sem=send_sem,
            recv_sem=recv_sem,
            device_id=where,
            device_id_type=MESH,
        )

    def near_plane(par, side):
        return to_neighbour(
            side, PS.at[par], PN.at[par, side], ns_sem.at[side], nr_sem.at[par, max(side - 1, 0)]
        )

    def halo(par, side):
        if side < 2:
            src = SC.at[side] if par else U.at[par, :, :, cd if side == 0 else 1]
            dst = U.at[par, :, :, 0 if side == 0 else cd + 1]
        else:
            src, dst = SS.at[par, side - 2], SR.at[par, side - 2]
        return to_neighbour(side, src, dst, hs_sem.at[side], hr_sem.at[par, side])

    sends = (None, None, has_high, has_low)
    takes = (None, None, has_low, has_high)

    def guarded(condition, act):
        if condition is None:
            act()
        else:
            pl.when(condition)(act)

    def start_all(make, par):
        for side in range(4):
            guarded(sends[side], lambda side=side: make(par, side).start())

    def take_planes(par):
        both = pltpu.make_async_remote_copy(
            src_ref=PN.at[par, pl.ds(0, 2)],
            dst_ref=PN.at[par, pl.ds(0, 2)],
            send_sem=ns_sem.at[0],
            recv_sem=nr_sem.at[par, 0],
            device_id={"circ": c_low},
            device_id_type=MESH,
        )
        both.wait_recv()
        for side in (2, 3):
            guarded(takes[side], lambda side=side: near_plane(par, side).wait_recv())

    def take_halos(par):
        for side in range(4):
            guarded(takes[side], lambda side=side: halo(par, side).wait_recv())

    def drain_all(make, par):
        for side in range(4):
            guarded(sends[side], lambda side=side: make(par, side).wait_send())

    def pack_span(par):
        for f in range(5):
            for h in range(2):
                cells = U[par, f, h, own]
                SS[par, 0, f, h] = cells[:, 15]
                SS[par, 1, f, h] = cells[:, 0]

    def mirror_span(par):
        def hub():
            for f in range(5):
                for h in range(2):
                    edge = SS[par, 1, f, h]
                    SR[par, 0, f, h] = -edge if f == 3 else edge

        def casing():
            for f in range(5):
                for h in range(2):
                    edge = SS[par, 0, f, h]
                    SR[par, 1, f, h] = -edge if f == 3 else edge

        pl.when(jnp.logical_not(has_low))(hub)
        pl.when(jnp.logical_not(has_high))(casing)

    def compact_base(par, ends, nexts, force):
        prims = derived(ends)
        stack = PS[par]
        c_lo, c_hi, s_lo, s_hi = (PN[par, k] for k in range(4))
        field = lax.broadcasted_iota(jnp.int32, (5, LANES), 0)
        mirror = jnp.where(field == 3, -stack, stack)
        place = lane % 16
        below = pltpu.roll(jnp.where(lane >= LANES - 16, c_lo, stack), 16, 1)
        above = pltpu.roll(jnp.where(lane < 16, c_hi, stack), LANES - 16, 1)
        low = jnp.where(has_low, pltpu.roll(s_lo, LANES - 15, 1), mirror)
        left = jnp.where(place == 0, low, pltpu.roll(stack, 1, 1))
        high = jnp.where(has_high, pltpu.roll(s_hi, 15, 1), mirror)
        right = jnp.where(place == 15, high, pltpu.roll(stack, LANES - 1, 1))
        below, above, left, right = (lines_of(x) for x in (below, above, left, right))

        def whole(cells, direction):
            return along(cells, derived(cells), direction)

        mid = [along(ends, prims, d) for d in range(3)]
        c_up = twice_flux(mid[1], whole(above, 1), 1)
        c_dn = twice_flux(whole(below, 1), mid[1], 1)
        s_up = twice_flux(mid[2], whole(right, 2), 2)
        s_dn = twice_flux(whole(left, 2), mid[2], 2)
        other = [jnp.where(rotor, b, a) for a, b in zip(ends, nexts)]
        inner = [jnp.where(rotor, a, b) for a, b in zip(ends, nexts)]
        axial = twice_flux(whole(other, 0), whole(inner, 0), 0)
        sign = jnp.where(rotor, 1.0, -1.0)
        div = [
            (c_up[j] - c_dn[j]) + (s_up[j] - s_dn[j]) - sign * axial[j] for j in range(5)
        ]
        return advanced(ends, div, source(ends, force))

    def compact_finish(par, ends, base):
        turn = off_s[par]
        turn = jnp.where(rotor, turn, cycle - turn)
        start = lax.rem(circ * cd + turn - 1 + cycle, cycle)
        taps = [jnp.full((5, LANES), wts_s[par, k], F32) for k in range(4)]
        scale = 1.0 / ((taps[0] + taps[1]) + (taps[2] + taps[3]))
        ghost = jnp.zeros((5, LANES), F32)
        for k in range(4):
            place = start + k
            sector = lax.rem(place // cd, sectors)
            back = LANES - 16 * lax.rem(place, cd)
            turned = lax.rem(back, LANES)
            first = pltpu.roll(PR[par][sector], turned, 1)
            second = pltpu.roll(PR[par][lax.rem(sector + 1, sectors)], turned, 1)
            ghost = ghost + (taps[k] * scale) * jnp.where(lane < back, first, second)
        ghost = lines_of(ghost)
        left = [jnp.where(rotor, a, b) for a, b in zip(ends, ghost)]
        right = [jnp.where(rotor, b, a) for a, b in zip(ends, ghost)]
        plane = twice_flux(
            along(left, derived(left), 0), along(right, derived(right), 0), 0
        )
        for j in range(5):
            PF[0, par, j] = to_tile(0.5 * plane[j])[:, :16]
        step = jnp.where(rotor, -HALF_STEP, HALF_STEP)
        return [base[j] + step * plane[j] for j in range(5)]

    def insert(lines, dest):
        tile = jnp.broadcast_to(lines[0], (8, LANES))
        for f in range(1, 5):
            tile = jnp.where(sub8 == f, lines[f], tile)
        turned = jnp.transpose(tile)
        here = lax.broadcasted_iota(jnp.int32, (16, LANES), 1) == jnp.where(rotor, 127, 0)
        for f in range(5):
            for c in range(cd):
                column = jnp.broadcast_to(turned[16 * c : 16 * c + 16, f : f + 1], (16, LANES))
                dest(f, c, here, column)

    def prim_rows(par, first, last):
        def one(c, _):
            for h in range(2):
                values = derived([U[par, f, h, c] for f in range(5)])
                for k in range(5):
                    W[k, h, c] = values[k]
            return _

        lax.fori_loop(first, last, one, 0)

    lane16 = lax.broadcasted_iota(jnp.int32, (16, LANES), 1)
    sub16 = lax.broadcasted_iota(jnp.int32, (16, LANES), 0)

    def bulk(par, store):
        def state_at(c):
            return [
                ([U[par, f, h, c] for f in range(5)], [W[k, h, c] for k in range(5)])
                for h in range(2)
            ]

        def one(c, lower, last_row):
            here = state_at(c + 1)
            if last_row:
                upper = None
                div = [[-lower[h][j] for j in range(5)] for h in range(2)]
            else:
                there = state_at(c + 2)
                upper = tuple(
                    tuple(twice_flux(along(*here[h], 1), along(*there[h], 1), 1))
                    for h in range(2)
                )
                div = [[upper[h][j] - lower[h][j] for j in range(5)] for h in range(2)]

            full = [along(*here[h], 0) for h in range(2)]

            def before(pick, inlet):
                turned = [pltpu.roll(pick(full[h]), 1, 1) for h in range(2)]
                return (
                    jnp.where(lane16 == 0, inlet, turned[0]),
                    jnp.where(lane16 == 0, turned[0], turned[1]),
                )

            cells = [before(lambda s, f=f: s[0][f], INLET[f]) for f in range(5)]
            u = before(lambda s: s[1], INLET_U)
            p = before(lambda s: s[2], INLET_P)
            a = before(lambda s: s[3], INLET_U + INLET_SOUND)
            flux = [
                twice_flux(([x[h] for x in cells], u[h], p[h], a[h]), full[h], 0)
                for h in range(2)
            ]
            last = twice_flux(full[1], full[1], 0)
            for j in range(5):
                turned = [pltpu.roll(flux[h][j], LANES - 1, 1) for h in range(2)]
                div[0][j] += jnp.where(lane16 == 127, turned[1], turned[0]) - flux[0][j]
                div[1][j] += jnp.where(lane16 == 127, last[j], turned[1]) - flux[1][j]

            for h in range(2):
                full = along(*here[h], 2)
                flux = twice_flux(
                    (
                        [pltpu.roll(full[0][f], 1, 0) for f in range(5)],
                        pltpu.roll(full[1], 1, 0),
                        pltpu.roll(full[2], 1, 0),
                        pltpu.roll(full[3], 1, 0),
                    ),
                    full,
                    2,
                )
                for j in range(5):
                    inside = jnp.where(sub16 == 0, 0.0, flux[j])
                    div[h][j] += pltpu.roll(inside, 15, 0) - inside
                force = [FO[d, h, c] for d in range(3)]
                new = advanced(here[h][0], div[h], source(here[h][0], force))
                for j in range(5):
                    store(j, h, c, new[j])
            return upper

        none = jnp.zeros((16, LANES), F32)
        start = tuple(tuple(none for _ in range(5)) for _ in range(2))
        final = lax.fori_loop(0, cd - 1, lambda c, lower: one(c, lower, False), start)
        one(cd - 1, final, True)

    def edges(par, shift):
        def flux_of(low, high, direction):
            return twice_flux(
                along(low, derived(low), direction),
                along(high, derived(high), direction),
                direction,
            )

        for h in range(2):
            rows = [[U[par, f, h, c] for f in range(5)] for c in (0, 1, cd, cd + 1)]
            low = flux_of(rows[0], rows[1], 1)
            high = flux_of(rows[2], rows[3], 1)
            for j in range(5):
                shift(j, h, 0, pl.ds(0, 16), HALF_STEP * low[j])
                shift(j, h, cd - 1, pl.ds(0, 16), -HALF_STEP * high[j])
            bottom, top = ([SS[par, k, f, h] for f in range(5)] for k in (1, 0))
            below, above = ([SR[par, k, f, h] for f in range(5)] for k in (0, 1))
            low = flux_of(below, bottom, 2)
            high = flux_of(top, above, 2)
            for j in range(5):
                shift(j, h, pl.ds(0, cd), 0, HALF_STEP * low[j])
                shift(j, h, pl.ds(0, cd), 15, -HALF_STEP * high[j])

    def blocks_of(ref):
        return [ref(f).reshape(cd * 16, LANES) for f in range(5)]

    loaded(U.at[0, :, half, own], 0)
    (ends, nexts) = end_layers(blocks_of(lambda f: U[0, f, half, own]))

    def conserved(raw):
        r, v0, v1, v2, p = raw
        return [r, r * v0, r * v1, r * v2, p * 2.5 + 0.5 * r * (v0 * v0 + v1 * v1 + v2 * v2)]

    ends, nexts = conserved(ends), conserved(nexts)
    put_lines(0, ends)
    loaded(U.at[0, :, row, own], 1)
    loaded(FO, 2)
    load_offsets.wait()
    load_weights.wait()
    lax.fori_loop(1, cd + 1, conserve, 0)
    pack_span(0)
    force, _ = end_layers([FO[d, half].reshape(cd * 16, LANES) for d in range(3)])
    prim_rows(0, 1, cd + 1)
    peers = sectors + 2 + has_low.astype(jnp.int32) + has_high.astype(jnp.int32)
    pl.semaphore_wait(barrier, peers)
    for copy in plane_copies(0):
        copy.start()
    start_all(near_plane, 0)
    start_all(halo, 0)
    mirror_span(0)

    def keep(j, h, c, value):
        U[1, j, h, c + 1] = value

    bulk(0, keep)
    def shift_state(j, h, c, s, value):
        c = pl.ds(1, cd) if isinstance(c, pl.Slice) else c + 1
        U[1, j, h, c, s] = U[1, j, h, c, s] + value

    def halo_part():
        take_halos(0)
        edges(0, shift_state)
        pack_span(1)
        for f in range(5):
            for h in range(2):
                SC[0, f, h] = U[1, f, h, cd]
                SC[1, f, h] = U[1, f, h, 1]
        drain_all(halo, 0)
        start_all(halo, 1)
        mirror_span(1)

    pl.when(rotor)(halo_part)
    take_planes(0)
    base = compact_base(0, ends, nexts, force)
    all_planes(0).wait_recv()
    ends = compact_finish(0, ends, base)
    put_lines(1, ends)
    drain_all(near_plane, 0)
    start_all(near_plane, 1)
    for copy in plane_copies(1):
        copy.start()
    pl.when(jnp.logical_not(rotor))(halo_part)

    def into_state(f, c, here, column):
        U[1, f, half, c + 1] = jnp.where(here, column, U[1, f, half, c + 1])

    insert(ends, into_state)

    _, nexts = end_layers(blocks_of(lambda f: U[1, f, half, own]))
    prim_rows(1, 1, cd + 1)

    def emit(j, h, c, value):
        OB[0, j, c, :, h * LANES : (h + 1) * LANES] = value

    bulk(1, emit)
    take_halos(1)

    def shift_out(j, h, c, s, value):
        lanes = pl.ds(h * LANES, LANES)
        OB[0, j, c, s, lanes] = OB[0, j, c, s, lanes] + value

    edges(1, shift_out)
    take_planes(1)
    base = compact_base(1, ends, nexts, force)
    all_planes(0).wait_send()
    all_planes(1).wait_send()
    drain_all(near_plane, 1)
    drain_all(halo, 1)
    all_planes(1).wait_recv()
    ends = compact_finish(1, ends, base)

    def into_out(f, c, here, column):
        lanes = pl.ds(pl.multiple_of(half * LANES, LANES), LANES)
        OB[0, f, c, :, lanes] = jnp.where(here, column, OB[0, f, c, :, lanes])

    insert(ends, into_out)


def write_out(state, plane, out, plane_out, sems):
    writes = [
        pltpu.make_async_copy(state, out, sems.at[0]),
        pltpu.make_async_copy(plane, plane_out, sems.at[1]),
    ]
    for copy in writes:
        copy.start()
    for copy in writes:
        copy.wait()


def solution(mesh):
    sectors = mesh.shape["circ"]
    bands = mesh.shape["span"]

    def body(density, velocity, pressure, blade_force, offsets, weights):
        _, cd, sd, axial = density.shape
        vmem, dma = pltpu.VMEM, pltpu.SemaphoreType.DMA
        any_space = pl.BlockSpec(memory_space=pl.ANY)
        in_vmem = pl.BlockSpec(memory_space=pltpu.VMEM)
        results = pl.pallas_call(
            functools.partial(kernel, sectors, bands),
            out_shape=(
                vmem((1, 5, cd, sd, axial), F32),
                vmem((1, 2, 5, cd, sd), F32),
            ),
            in_specs=[any_space] * 6,
            out_specs=(in_vmem, in_vmem),
            scratch_shapes=[
                vmem((2, 5, 2, cd + 2, sd, LANES), F32),
                vmem((5, 2, cd + 2, sd, LANES), F32),
                vmem((3, 2, cd, sd, LANES), F32),
                vmem((2, 2, 5, 2, cd, LANES), F32),
                vmem((2, 2, 5, 2, cd, LANES), F32),
                vmem((2, 5, 2, sd, LANES), F32),
                vmem((2, 5, LANES), F32),
                vmem((sectors, 5, LANES), F32),
                vmem((sectors, 5, LANES), F32),
                vmem((2, 4, 5, LANES), F32),
                pltpu.SMEM((2,), jnp.int32),
                pltpu.SMEM((2, 4), F32),
                dma((5,)),
                dma((2,)),
                dma((2,)),
                dma((4,)),
                dma((2, 3)),
                dma((4,)),
                dma((2, 4)),
            ],
            compiler_params=pltpu.CompilerParams(collective_id=0, has_side_effects=True),
        )(density, velocity, pressure, blade_force, offsets, weights)
        results = [pltpu.with_memory_space_constraint(x, pltpu.VMEM) for x in results]
        return pl.pallas_call(
            write_out,
            out_shape=(
                jax.ShapeDtypeStruct((1, 5, cd, sd, axial), F32),
                jax.ShapeDtypeStruct((1, 2, 5, cd, sd), F32),
            ),
            in_specs=[in_vmem, in_vmem],
            out_specs=(any_space, any_space),
            scratch_shapes=[dma((2,))],
        )(*results)

    placed = (
        P("row", "circ", "span", None),
        P("row", None, "circ", "span", None),
        P("row", "circ", "span", None),
        P("row", None, "circ", "span", None),
        P(),
        P(),
    )
    return jax.shard_map(
        body,
        mesh=mesh,
        in_specs=placed,
        out_specs=(P("row", None, "circ", "span", None), P("row", None, None, "circ", "span")),
        check_vma=False,
    )
```

```python
import functools
import math

import jax
import jax.numpy as jnp
from jax import lax
from jax.experimental import pallas as pl
from jax.experimental.pallas import tpu as pltpu
from jax.sharding import PartitionSpec as P

F32 = jnp.float32
MESH = pl.DeviceIdType.MESH
TIME_STEP = 0.04
HALF_STEP = 0.5 * TIME_STEP
LANES = 128
INLET = (1.0, 0.5, 0.0, 0.0, 2.625)
INLET_U = 0.5
INLET_P = 1.0
INLET_SOUND = math.sqrt(1.4)


def derived(cells):
    density, m0, m1, m2, energy = cells
    inverse = 1.0 / density
    u0, u1, u2 = m0 * inverse, m1 * inverse, m2 * inverse
    pressure = 0.4 * (energy - 0.5 * (m0 * u0 + m1 * u1 + m2 * u2))
    sound = jnp.sqrt(1.4 * pressure * inverse)
    return (u0, u1, u2, pressure, sound)


def twice_flux(left, right, direction):
    cells_l, u_l, p_l, a_l = left
    cells_r, u_r, p_r, a_r = right
    speed = jnp.maximum(a_l, a_r)
    up, down = u_l + speed, u_r - speed
    out = [cells_l[j] * up + cells_r[j] * down for j in range(5)]
    out[1 + direction] = out[1 + direction] + (p_l + p_r)
    out[4] = out[4] + (p_l * u_l + p_r * u_r)
    return out


def along(cells, prims, direction):
    normal = prims[direction]
    return (cells, normal, prims[3], jnp.abs(normal) + prims[4])


def source(cells, force):
    return [
        None,
        cells[0] * force[0],
        cells[0] * force[1],
        cells[0] * force[2],
        cells[1] * force[0] + cells[2] * force[1] + cells[3] * force[2],
    ]


def advanced(cells, div, src):
    out = []
    for j in range(5):
        value = cells[j] - HALF_STEP * div[j]
        if src[j] is not None:
            value = value + TIME_STEP * src[j]
        out.append(value)
    return out


def kernel(
    sectors,
    bands,
    dens,
    vel,
    pres,
    forc,
    offs,
    wts,
    OB,
    PF,
    U,
    W,
    FO,
    SS,
    SR,
    SC,
    PS,
    PR0,
    PR1,
    PN,
    off_s,
    wts_s,
    in_sem,
    ps_sem,
    pr_sem,
    ns_sem,
    nr_sem,
    hs_sem,
    hr_sem,
):
    row = lax.axis_index("row")
    circ = lax.axis_index("circ")
    span = lax.axis_index("span")
    cd = FO.shape[2]
    cycle = sectors * cd
    c_low, c_high = lax.rem(circ + sectors - 1, sectors), lax.rem(circ + 1, sectors)
    has_low, has_high = span > 0, span < bands - 1
    rotor = row == 0
    half = 1 - row

    own = pl.ds(1, cd)
    PR = (PR0, PR1)

    def load_half(h, sem):
        lanes = pl.ds(pl.multiple_of(h * LANES, LANES), LANES)
        for src, dst in (
            (dens.at[0, :, :, lanes], U.at[0, 0, h, own]),
            (vel.at[0, :, :, :, lanes], U.at[0, pl.ds(1, 3), h, own]),
            (pres.at[0, :, :, lanes], U.at[0, 4, h, own]),
        ):
            pltpu.make_async_copy(src, dst, in_sem.at[sem]).start()

    def loaded(ref, sem):
        pltpu.make_async_copy(ref, ref, in_sem.at[sem]).wait()

    load_half(half, 0)
    barrier = pltpu.get_barrier_semaphore()
    for i in range(sectors):
        q = lax.rem(circ + sectors // 2 + i, sectors)
        pl.semaphore_signal(
            barrier, inc=1, device_id={"row": 1 - row, "circ": q}, device_id_type=MESH
        )
    for q in (c_low, c_high):
        pl.semaphore_signal(barrier, inc=1, device_id={"circ": q}, device_id_type=MESH)

    @pl.when(has_low)
    def _():
        pl.semaphore_signal(barrier, inc=1, device_id={"span": span - 1}, device_id_type=MESH)

    @pl.when(has_high)
    def _():
        pl.semaphore_signal(barrier, inc=1, device_id={"span": span + 1}, device_id_type=MESH)

    load_half(row, 1)
    for h in range(2):
        lanes = pl.ds(h * LANES, LANES)
        pltpu.make_async_copy(forc.at[0, :, :, :, lanes], FO.at[:, h], in_sem.at[2]).start()
    load_offsets = pltpu.make_async_copy(offs, off_s, in_sem.at[3])
    load_weights = pltpu.make_async_copy(wts, wts_s, in_sem.at[4])
    load_offsets.start()
    load_weights.start()

    lane = lax.broadcasted_iota(jnp.int32, (5, LANES), 1)
    sub8 = lax.broadcasted_iota(jnp.int32, (8, LANES), 0)

    def conserve(c, _):
        for h in range(2):
            r = U[0, 0, h, c]
            v = [U[0, 1 + d, h, c] for d in range(3)]
            p = U[0, 4, h, c]
            for d in range(3):
                U[0, 1 + d, h, c] = r * v[d]
            U[0, 4, h, c] = p * 2.5 + 0.5 * r * (v[0] * v[0] + v[1] * v[1] + v[2] * v[2])
        return _

    def to_tile(line):
        tile = jnp.broadcast_to(line, (8, LANES))
        for bit in (4, 2, 1):
            tile = jnp.where((sub8 & bit) != 0, pltpu.roll(tile, LANES - 16 * bit, 1), tile)
        return tile

    def end_layers(block_of):
        ends, nexts = [], []
        for turned in (jnp.transpose(b) for b in block_of):
            ends.append(jnp.where(rotor, turned[127:128], turned[0:1]))
            nexts.append(jnp.where(rotor, turned[126:127], turned[1:2]))
        return ends, nexts

    def put_lines(par, lines):
        for f in range(5):
            PS[par, f : f + 1] = lines[f]

    def lines_of(stack):
        return [stack[f : f + 1] for f in range(5)]

    def plane_copies(par):
        copies = []
        for i in range(sectors):
            q = lax.rem(circ + sectors // 2 + i, sectors)
            copies.append(
                pltpu.make_async_remote_copy(
                    src_ref=PS.at[par],
                    dst_ref=PR[par].at[circ],
                    send_sem=ps_sem.at[par],
                    recv_sem=pr_sem.at[par],
                    device_id={"row": 1 - row, "circ": q},
                    device_id_type=MESH,
                )
            )
        return copies

    def all_planes(par):
        return pltpu.make_async_remote_copy(
            src_ref=PR[par],
            dst_ref=PR[par],
            send_sem=ps_sem.at[par],
            recv_sem=pr_sem.at[par],
            device_id={"row": 1 - row},
            device_id_type=MESH,
        )

    def to_neighbour(side, src, dst, send_sem, recv_sem):
        where = (
            {"circ": c_high},
            {"circ": c_low},
            {"span": span + 1},
            {"span": span - 1},
        )[side]
        return pltpu.make_async_remote_copy(
            src_ref=src,
            dst_ref=dst,
            send_sem=send_sem,
            recv_sem=recv_sem,
            device_id=where,
            device_id_type=MESH,
        )

    def near_plane(par, side):
        return to_neighbour(
            side, PS.at[par], PN.at[par, side], ns_sem.at[side], nr_sem.at[par, max(side - 1, 0)]
        )

    def halo(par, side):
        if side < 2:
            src = SC.at[side] if par else U.at[par, :, :, cd if side == 0 else 1]
            dst = U.at[par, :, :, 0 if side == 0 else cd + 1]
        else:
            src, dst = SS.at[par, side - 2], SR.at[par, side - 2]
        return to_neighbour(side, src, dst, hs_sem.at[side], hr_sem.at[par, side])

    sends = (None, None, has_high, has_low)
    takes = (None, None, has_low, has_high)

    def guarded(condition, act):
        if condition is None:
            act()
        else:
            pl.when(condition)(act)

    def start_all(make, par):
        for side in range(4):
            guarded(sends[side], lambda side=side: make(par, side).start())

    def take_planes(par):
        both = pltpu.make_async_remote_copy(
            src_ref=PN.at[par, pl.ds(0, 2)],
            dst_ref=PN.at[par, pl.ds(0, 2)],
            send_sem=ns_sem.at[0],
            recv_sem=nr_sem.at[par, 0],
            device_id={"circ": c_low},
            device_id_type=MESH,
        )
        both.wait_recv()
        for side in (2, 3):
            guarded(takes[side], lambda side=side: near_plane(par, side).wait_recv())

    def take_halos(par):
        for side in range(4):
            guarded(takes[side], lambda side=side: halo(par, side).wait_recv())

    def drain_all(make, par):
        for side in range(4):
            guarded(sends[side], lambda side=side: make(par, side).wait_send())

    def pack_span(par):
        for f in range(5):
            for h in range(2):
                cells = U[par, f, h, own]
                SS[par, 0, f, h] = cells[:, 15]
                SS[par, 1, f, h] = cells[:, 0]

    def mirror_span(par):
        def hub():
            for f in range(5):
                for h in range(2):
                    edge = SS[par, 1, f, h]
                    SR[par, 0, f, h] = -edge if f == 3 else edge

        def casing():
            for f in range(5):
                for h in range(2):
                    edge = SS[par, 0, f, h]
                    SR[par, 1, f, h] = -edge if f == 3 else edge

        pl.when(jnp.logical_not(has_low))(hub)
        pl.when(jnp.logical_not(has_high))(casing)

    def compact_base(par, ends, nexts, force):
        prims = derived(ends)
        stack = PS[par]
        c_lo, c_hi, s_lo, s_hi = (PN[par, k] for k in range(4))
        field = lax.broadcasted_iota(jnp.int32, (5, LANES), 0)
        mirror = jnp.where(field == 3, -stack, stack)
        place = lane % 16
        below = pltpu.roll(jnp.where(lane >= LANES - 16, c_lo, stack), 16, 1)
        above = pltpu.roll(jnp.where(lane < 16, c_hi, stack), LANES - 16, 1)
        low = jnp.where(has_low, pltpu.roll(s_lo, LANES - 15, 1), mirror)
        left = jnp.where(place == 0, low, pltpu.roll(stack, 1, 1))
        high = jnp.where(has_high, pltpu.roll(s_hi, 15, 1), mirror)
        right = jnp.where(place == 15, high, pltpu.roll(stack, LANES - 1, 1))
        below, above, left, right = (lines_of(x) for x in (below, above, left, right))

        def whole(cells, direction):
            return along(cells, derived(cells), direction)

        mid = [along(ends, prims, d) for d in range(3)]
        c_up = twice_flux(mid[1], whole(above, 1), 1)
        c_dn = twice_flux(whole(below, 1), mid[1], 1)
        s_up = twice_flux(mid[2], whole(right, 2), 2)
        s_dn = twice_flux(whole(left, 2), mid[2], 2)
        other = [jnp.where(rotor, b, a) for a, b in zip(ends, nexts)]
        inner = [jnp.where(rotor, a, b) for a, b in zip(ends, nexts)]
        axial = twice_flux(whole(other, 0), whole(inner, 0), 0)
        sign = jnp.where(rotor, 1.0, -1.0)
        div = [
            (c_up[j] - c_dn[j]) + (s_up[j] - s_dn[j]) - sign * axial[j] for j in range(5)
        ]
        return advanced(ends, div, source(ends, force))

    def compact_finish(par, ends, base):
        turn = off_s[par]
        turn = jnp.where(rotor, turn, cycle - turn)
        start = lax.rem(circ * cd + turn - 1 + cycle, cycle)
        taps = [jnp.full((5, LANES), wts_s[par, k], F32) for k in range(4)]
        scale = 1.0 / ((taps[0] + taps[1]) + (taps[2] + taps[3]))
        ghost = jnp.zeros((5, LANES), F32)
        for k in range(4):
            place = start + k
            sector = lax.rem(place // cd, sectors)
            back = LANES - 16 * lax.rem(place, cd)
            turned = lax.rem(back, LANES)
            first = pltpu.roll(PR[par][sector], turned, 1)
            second = pltpu.roll(PR[par][lax.rem(sector + 1, sectors)], turned, 1)
            ghost = ghost + (taps[k] * scale) * jnp.where(lane < back, first, second)
        ghost = lines_of(ghost)
        left = [jnp.where(rotor, a, b) for a, b in zip(ends, ghost)]
        right = [jnp.where(rotor, b, a) for a, b in zip(ends, ghost)]
        plane = twice_flux(
            along(left, derived(left), 0), along(right, derived(right), 0), 0
        )
        step = jnp.where(rotor, -HALF_STEP, HALF_STEP)
        return plane, [base[j] + step * plane[j] for j in range(5)]

    def put_plane(par, plane):
        for j in range(5):
            PF[0, par, j] = to_tile(0.5 * plane[j])[:, :16]

    def insert(lines, dest):
        tile = jnp.broadcast_to(lines[0], (8, LANES))
        for f in range(1, 5):
            tile = jnp.where(sub8 == f, lines[f], tile)
        turned = jnp.transpose(tile)
        here = lax.broadcasted_iota(jnp.int32, (16, LANES), 1) == jnp.where(rotor, 127, 0)
        for f in range(5):
            for c in range(cd):
                column = jnp.broadcast_to(turned[16 * c : 16 * c + 16, f : f + 1], (16, LANES))
                dest(f, c, here, column)

    def prim_rows(par, first, last):
        def one(c, _):
            for h in range(2):
                values = derived([U[par, f, h, c] for f in range(5)])
                for k in range(5):
                    W[k, h, c] = values[k]
            return _

        lax.fori_loop(first, last, one, 0)

    lane16 = lax.broadcasted_iota(jnp.int32, (16, LANES), 1)
    sub16 = lax.broadcasted_iota(jnp.int32, (16, LANES), 0)

    def bulk(par, store):
        def state_at(c):
            return [
                ([U[par, f, h, c] for f in range(5)], [W[k, h, c] for k in range(5)])
                for h in range(2)
            ]

        def one(c, lower, last_row):
            here = state_at(c + 1)
            if last_row:
                upper = None
                div = [[-lower[h][j] for j in range(5)] for h in range(2)]
            else:
                there = state_at(c + 2)
                upper = tuple(
                    tuple(twice_flux(along(*here[h], 1), along(*there[h], 1), 1))
                    for h in range(2)
                )
                div = [[upper[h][j] - lower[h][j] for j in range(5)] for h in range(2)]

            full = [along(*here[h], 0) for h in range(2)]

            def before(pick, inlet):
                turned = [pltpu.roll(pick(full[h]), 1, 1) for h in range(2)]
                return (
                    jnp.where(lane16 == 0, inlet, turned[0]),
                    jnp.where(lane16 == 0, turned[0], turned[1]),
                )

            cells = [before(lambda s, f=f: s[0][f], INLET[f]) for f in range(5)]
            u = before(lambda s: s[1], INLET_U)
            p = before(lambda s: s[2], INLET_P)
            a = before(lambda s: s[3], INLET_U + INLET_SOUND)
            flux = [
                twice_flux(([x[h] for x in cells], u[h], p[h], a[h]), full[h], 0)
                for h in range(2)
            ]
            last = twice_flux(full[1], full[1], 0)
            for j in range(5):
                turned = [pltpu.roll(flux[h][j], LANES - 1, 1) for h in range(2)]
                div[0][j] += jnp.where(lane16 == 127, turned[1], turned[0]) - flux[0][j]
                div[1][j] += jnp.where(lane16 == 127, last[j], turned[1]) - flux[1][j]

            for h in range(2):
                full = along(*here[h], 2)
                flux = twice_flux(
                    (
                        [pltpu.roll(full[0][f], 1, 0) for f in range(5)],
                        pltpu.roll(full[1], 1, 0),
                        pltpu.roll(full[2], 1, 0),
                        pltpu.roll(full[3], 1, 0),
                    ),
                    full,
                    2,
                )
                for j in range(5):
                    inside = jnp.where(sub16 == 0, 0.0, flux[j])
                    div[h][j] += pltpu.roll(inside, 15, 0) - inside
                force = [FO[d, h, c] for d in range(3)]
                new = advanced(here[h][0], div[h], source(here[h][0], force))
                for j in range(5):
                    store(j, h, c, new[j])
            return upper

        none = jnp.zeros((16, LANES), F32)
        start = tuple(tuple(none for _ in range(5)) for _ in range(2))
        final = lax.fori_loop(0, cd - 1, lambda c, lower: one(c, lower, False), start)
        one(cd - 1, final, True)

    def edges(par, shift):
        def flux_of(low, high, direction):
            return twice_flux(
                along(low, derived(low), direction),
                along(high, derived(high), direction),
                direction,
            )

        for h in range(2):
            rows = [[U[par, f, h, c] for f in range(5)] for c in (0, 1, cd, cd + 1)]
            low = flux_of(rows[0], rows[1], 1)
            high = flux_of(rows[2], rows[3], 1)
            for j in range(5):
                shift(j, h, 0, pl.ds(0, 16), HALF_STEP * low[j])
                shift(j, h, cd - 1, pl.ds(0, 16), -HALF_STEP * high[j])
            bottom, top = ([SS[par, k, f, h] for f in range(5)] for k in (1, 0))
            below, above = ([SR[par, k, f, h] for f in range(5)] for k in (0, 1))
            low = flux_of(below, bottom, 2)
            high = flux_of(top, above, 2)
            for j in range(5):
                shift(j, h, pl.ds(0, cd), 0, HALF_STEP * low[j])
                shift(j, h, pl.ds(0, cd), 15, -HALF_STEP * high[j])

    def blocks_of(ref):
        return [ref(f).reshape(cd * 16, LANES) for f in range(5)]

    loaded(U.at[0, :, half, own], 0)
    (ends, nexts) = end_layers(blocks_of(lambda f: U[0, f, half, own]))

    def conserved(raw):
        r, v0, v1, v2, p = raw
        return [r, r * v0, r * v1, r * v2, p * 2.5 + 0.5 * r * (v0 * v0 + v1 * v1 + v2 * v2)]

    ends, nexts = conserved(ends), conserved(nexts)
    put_lines(0, ends)
    loaded(U.at[0, :, row, own], 1)
    loaded(FO, 2)
    load_offsets.wait()
    load_weights.wait()
    lax.fori_loop(1, cd + 1, conserve, 0)
    pack_span(0)
    force, _ = end_layers([FO[d, half].reshape(cd * 16, LANES) for d in range(3)])
    prim_rows(0, 1, cd + 1)
    peers = sectors + 2 + has_low.astype(jnp.int32) + has_high.astype(jnp.int32)
    pl.semaphore_wait(barrier, peers)
    for copy in plane_copies(0):
        copy.start()
    start_all(near_plane, 0)
    start_all(halo, 0)
    mirror_span(0)

    def keep(j, h, c, value):
        U[1, j, h, c + 1] = value

    bulk(0, keep)
    def shift_state(j, h, c, s, value):
        c = pl.ds(1, cd) if isinstance(c, pl.Slice) else c + 1
        U[1, j, h, c, s] = U[1, j, h, c, s] + value

    def halo_part():
        take_halos(0)
        edges(0, shift_state)
        drain_all(halo, 0)
        pack_span(1)
        for f in range(5):
            for h in range(2):
                SC[0, f, h] = U[1, f, h, cd]
                SC[1, f, h] = U[1, f, h, 1]
        start_all(halo, 1)
        mirror_span(1)

    take_planes(0)
    base = compact_base(0, ends, nexts, force)
    drain_all(near_plane, 0)
    all_planes(0).wait_recv()
    plane, ends = compact_finish(0, ends, base)
    put_lines(1, ends)
    start_all(near_plane, 1)
    for copy in plane_copies(1):
        copy.start()
    halo_part()
    put_plane(0, plane)

    def into_state(f, c, here, column):
        U[1, f, half, c + 1] = jnp.where(here, column, U[1, f, half, c + 1])

    insert(ends, into_state)

    _, nexts = end_layers(blocks_of(lambda f: U[1, f, half, own]))
    prim_rows(1, 1, cd + 1)

    def emit(j, h, c, value):
        OB[0, j, c, :, h * LANES : (h + 1) * LANES] = value

    bulk(1, emit)
    take_planes(1)
    base = compact_base(1, ends, nexts, force)
    take_halos(1)

    def shift_out(j, h, c, s, value):
        lanes = pl.ds(h * LANES, LANES)
        OB[0, j, c, s, lanes] = OB[0, j, c, s, lanes] + value

    edges(1, shift_out)
    all_planes(0).wait_send()
    all_planes(1).wait_send()
    drain_all(near_plane, 1)
    drain_all(halo, 1)
    all_planes(1).wait_recv()
    plane, ends = compact_finish(1, ends, base)

    def into_out(f, c, here, column):
        lanes = pl.ds(pl.multiple_of(half * LANES, LANES), LANES)
        OB[0, f, c, :, lanes] = jnp.where(here, column, OB[0, f, c, :, lanes])

    insert(ends, into_out)
    put_plane(1, plane)


def write_out(state, plane, out, plane_out, sems):
    writes = [
        pltpu.make_async_copy(state, out, sems.at[0]),
        pltpu.make_async_copy(plane, plane_out, sems.at[1]),
    ]
    for copy in writes:
        copy.start()
    for copy in writes:
        copy.wait()


def solution(mesh):
    sectors = mesh.shape["circ"]
    bands = mesh.shape["span"]

    def body(density, velocity, pressure, blade_force, offsets, weights):
        _, cd, sd, axial = density.shape
        vmem, dma = pltpu.VMEM, pltpu.SemaphoreType.DMA
        any_space = pl.BlockSpec(memory_space=pl.ANY)
        in_vmem = pl.BlockSpec(memory_space=pltpu.VMEM)
        results = pl.pallas_call(
            functools.partial(kernel, sectors, bands),
            out_shape=(
                vmem((1, 5, cd, sd, axial), F32),
                vmem((1, 2, 5, cd, sd), F32),
            ),
            in_specs=[any_space] * 6,
            out_specs=(in_vmem, in_vmem),
            scratch_shapes=[
                vmem((2, 5, 2, cd + 2, sd, LANES), F32),
                vmem((5, 2, cd + 2, sd, LANES), F32),
                vmem((3, 2, cd, sd, LANES), F32),
                vmem((2, 2, 5, 2, cd, LANES), F32),
                vmem((2, 2, 5, 2, cd, LANES), F32),
                vmem((2, 5, 2, sd, LANES), F32),
                vmem((2, 5, LANES), F32),
                vmem((sectors, 5, LANES), F32),
                vmem((sectors, 5, LANES), F32),
                vmem((2, 4, 5, LANES), F32),
                pltpu.SMEM((2,), jnp.int32),
                pltpu.SMEM((2, 4), F32),
                dma((5,)),
                dma((2,)),
                dma((2,)),
                dma((4,)),
                dma((2, 3)),
                dma((4,)),
                dma((2, 4)),
            ],
            compiler_params=pltpu.CompilerParams(collective_id=0, has_side_effects=True),
        )(density, velocity, pressure, blade_force, offsets, weights)
        results = [pltpu.with_memory_space_constraint(x, pltpu.VMEM) for x in results]
        return pl.pallas_call(
            write_out,
            out_shape=(
                jax.ShapeDtypeStruct((1, 5, cd, sd, axial), F32),
                jax.ShapeDtypeStruct((1, 2, 5, cd, sd), F32),
            ),
            in_specs=[in_vmem, in_vmem],
            out_specs=(any_space, any_space),
            scratch_shapes=[dma((2,))],
        )(*results)

    placed = (
        P("row", "circ", "span", None),
        P("row", None, "circ", "span", None),
        P("row", "circ", "span", None),
        P("row", None, "circ", "span", None),
        P(),
        P(),
    )
    return jax.shard_map(
        body,
        mesh=mesh,
        in_specs=placed,
        out_specs=(P("row", None, "circ", "span", None), P("row", None, None, "circ", "span")),
        check_vma=False,
    )
```

```python
import functools
import math

import jax
import jax.numpy as jnp
from jax import lax
from jax.experimental import pallas as pl
from jax.experimental.pallas import tpu as pltpu
from jax.sharding import PartitionSpec as P

F32 = jnp.float32
MESH = pl.DeviceIdType.MESH
TIME_STEP = 0.04
HALF_STEP = 0.5 * TIME_STEP
LANES = 128
INLET = (1.0, 0.5, 0.0, 0.0, 2.625)
INLET_U = 0.5
INLET_P = 1.0
INLET_SOUND = math.sqrt(1.4)


def derived(cells):
    density, m0, m1, m2, energy = cells
    inverse = 1.0 / density
    u0, u1, u2 = m0 * inverse, m1 * inverse, m2 * inverse
    pressure = 0.4 * (energy - 0.5 * (m0 * u0 + m1 * u1 + m2 * u2))
    sound = jnp.sqrt(1.4 * pressure * inverse)
    return (u0, u1, u2, pressure, sound)


def twice_flux(left, right, direction):
    cells_l, u_l, p_l, a_l = left
    cells_r, u_r, p_r, a_r = right
    speed = jnp.maximum(a_l, a_r)
    up, down = u_l + speed, u_r - speed
    out = [cells_l[j] * up + cells_r[j] * down for j in range(5)]
    out[1 + direction] = out[1 + direction] + (p_l + p_r)
    out[4] = out[4] + (p_l * u_l + p_r * u_r)
    return out


def along(cells, prims, direction):
    normal = prims[direction]
    return (cells, normal, prims[3], jnp.abs(normal) + prims[4])


def source(cells, force):
    return [
        None,
        cells[0] * force[0],
        cells[0] * force[1],
        cells[0] * force[2],
        cells[1] * force[0] + cells[2] * force[1] + cells[3] * force[2],
    ]


def advanced(cells, div, src):
    out = []
    for j in range(5):
        value = cells[j] - HALF_STEP * div[j]
        if src[j] is not None:
            value = value + TIME_STEP * src[j]
        out.append(value)
    return out


def kernel(
    sectors,
    bands,
    dens,
    vel,
    pres,
    forc,
    offs,
    wts,
    OB,
    PF,
    U,
    W,
    FO,
    SS,
    SR,
    SC,
    PS,
    PR0,
    PR1,
    PN,
    off_s,
    wts_s,
    local_sem,
    pr_sem,
    nr_sem,
    hr_sem,
):
    row = lax.axis_index("row")
    circ = lax.axis_index("circ")
    span = lax.axis_index("span")
    cd = FO.shape[2]
    cycle = sectors * cd
    c_low, c_high = lax.rem(circ + sectors - 1, sectors), lax.rem(circ + 1, sectors)
    has_low, has_high = span > 0, span < bands - 1
    rotor = row == 0
    half = 1 - row

    own = pl.ds(1, cd)
    PR = (PR0, PR1)

    def load_half(h, sem):
        lanes = pl.ds(pl.multiple_of(h * LANES, LANES), LANES)
        for src, dst in (
            (dens.at[0, :, :, lanes], U.at[0, 0, h, own]),
            (vel.at[0, :, :, :, lanes], U.at[0, pl.ds(1, 3), h, own]),
            (pres.at[0, :, :, lanes], U.at[0, 4, h, own]),
        ):
            pltpu.make_async_copy(src, dst, local_sem.at[sem]).start()

    def loaded(ref, sem):
        pltpu.make_async_copy(ref, ref, local_sem.at[sem]).wait()

    load_half(half, 0)
    barrier = pltpu.get_barrier_semaphore()
    for i in range(sectors):
        q = lax.rem(circ + sectors // 2 + i, sectors)
        pl.semaphore_signal(
            barrier, inc=1, device_id={"row": 1 - row, "circ": q}, device_id_type=MESH
        )
    for q in (c_low, c_high):
        pl.semaphore_signal(barrier, inc=1, device_id={"circ": q}, device_id_type=MESH)

    @pl.when(has_low)
    def _():
        pl.semaphore_signal(barrier, inc=1, device_id={"span": span - 1}, device_id_type=MESH)

    @pl.when(has_high)
    def _():
        pl.semaphore_signal(barrier, inc=1, device_id={"span": span + 1}, device_id_type=MESH)

    load_half(row, 1)
    for h in range(2):
        lanes = pl.ds(h * LANES, LANES)
        pltpu.make_async_copy(forc.at[0, :, :, :, lanes], FO.at[:, h], local_sem.at[2]).start()
    load_offsets = pltpu.make_async_copy(offs, off_s, local_sem.at[3])
    load_weights = pltpu.make_async_copy(wts, wts_s, local_sem.at[4])
    load_offsets.start()
    load_weights.start()

    lane = lax.broadcasted_iota(jnp.int32, (5, LANES), 1)
    sub8 = lax.broadcasted_iota(jnp.int32, (8, LANES), 0)

    def conserve(c, _):
        for h in range(2):
            r = U[0, 0, h, c]
            v = [U[0, 1 + d, h, c] for d in range(3)]
            p = U[0, 4, h, c]
            for d in range(3):
                U[0, 1 + d, h, c] = r * v[d]
            U[0, 4, h, c] = p * 2.5 + 0.5 * r * (v[0] * v[0] + v[1] * v[1] + v[2] * v[2])
        return _

    def to_tile(line):
        tile = jnp.broadcast_to(line, (8, LANES))
        for bit in (4, 2, 1):
            tile = jnp.where((sub8 & bit) != 0, pltpu.roll(tile, LANES - 16 * bit, 1), tile)
        return tile

    def end_layers(block_of):
        ends, nexts = [], []
        for turned in (jnp.transpose(b) for b in block_of):
            ends.append(jnp.where(rotor, turned[127:128], turned[0:1]))
            nexts.append(jnp.where(rotor, turned[126:127], turned[1:2]))
        return ends, nexts

    def put_lines(par, lines):
        for f in range(5):
            PS[par, f : f + 1] = lines[f]

    def lines_of(stack):
        return [stack[f : f + 1] for f in range(5)]

    def plane_copies(par):
        copies = []
        for i in range(sectors):
            q = lax.rem(circ + sectors // 2 + i, sectors)
            copies.append(
                pltpu.make_async_remote_copy(
                    src_ref=PS.at[par],
                    dst_ref=PR[par].at[circ],
                    send_sem=local_sem.at[par],
                    recv_sem=pr_sem.at[par],
                    device_id={"row": 1 - row, "circ": q},
                    device_id_type=MESH,
                )
            )
        return copies

    def all_planes(par):
        return pltpu.make_async_remote_copy(
            src_ref=PR[par],
            dst_ref=PR[par],
            send_sem=local_sem.at[par],
            recv_sem=pr_sem.at[par],
            device_id={"row": 1 - row},
            device_id_type=MESH,
        )

    def to_neighbour(side, src, dst, send_sem, recv_sem):
        where = (
            {"circ": c_high},
            {"circ": c_low},
            {"span": span + 1},
            {"span": span - 1},
        )[side]
        return pltpu.make_async_remote_copy(
            src_ref=src,
            dst_ref=dst,
            send_sem=send_sem,
            recv_sem=recv_sem,
            device_id=where,
            device_id_type=MESH,
        )

    def near_plane(par, side):
        return to_neighbour(
            side, PS.at[par], PN.at[par, side], local_sem.at[2 + side], nr_sem.at[par, max(side - 1, 0)]
        )

    def halo(par, side):
        if side < 2:
            src = SC.at[side] if par else U.at[par, :, :, cd if side == 0 else 1]
            dst = U.at[par, :, :, 0 if side == 0 else cd + 1]
        else:
            src, dst = SS.at[par, side - 2], SR.at[par, side - 2]
        return to_neighbour(side, src, dst, local_sem.at[6 + side], hr_sem.at[par, side])

    sends = (None, None, has_high, has_low)
    takes = (None, None, has_low, has_high)

    def guarded(condition, act):
        if condition is None:
            act()
        else:
            pl.when(condition)(act)

    def start_all(make, par):
        for side in range(4):
            guarded(sends[side], lambda side=side: make(par, side).start())

    def take_planes(par):
        both = pltpu.make_async_remote_copy(
            src_ref=PN.at[par, pl.ds(0, 2)],
            dst_ref=PN.at[par, pl.ds(0, 2)],
            send_sem=local_sem.at[2],
            recv_sem=nr_sem.at[par, 0],
            device_id={"circ": c_low},
            device_id_type=MESH,
        )
        both.wait_recv()
        for side in (2, 3):
            guarded(takes[side], lambda side=side: near_plane(par, side).wait_recv())

    def take_halos(par):
        for side in range(4):
            guarded(takes[side], lambda side=side: halo(par, side).wait_recv())

    def drain_all(make, par):
        for side in range(4):
            guarded(sends[side], lambda side=side: make(par, side).wait_send())

    def pack_span(par):
        for f in range(5):
            for h in range(2):
                cells = U[par, f, h, own]
                SS[par, 0, f, h] = cells[:, 15]
                SS[par, 1, f, h] = cells[:, 0]

    def mirror_span(par):
        def hub():
            for f in range(5):
                for h in range(2):
                    edge = SS[par, 1, f, h]
                    SR[par, 0, f, h] = -edge if f == 3 else edge

        def casing():
            for f in range(5):
                for h in range(2):
                    edge = SS[par, 0, f, h]
                    SR[par, 1, f, h] = -edge if f == 3 else edge

        pl.when(jnp.logical_not(has_low))(hub)
        pl.when(jnp.logical_not(has_high))(casing)

    def compact_base(par, ends, nexts, force):
        prims = derived(ends)
        stack = PS[par]
        c_lo, c_hi, s_lo, s_hi = (PN[par, k] for k in range(4))
        field = lax.broadcasted_iota(jnp.int32, (5, LANES), 0)
        mirror = jnp.where(field == 3, -stack, stack)
        place = lane % 16
        below = pltpu.roll(jnp.where(lane >= LANES - 16, c_lo, stack), 16, 1)
        above = pltpu.roll(jnp.where(lane < 16, c_hi, stack), LANES - 16, 1)
        low = jnp.where(has_low, pltpu.roll(s_lo, LANES - 15, 1), mirror)
        left = jnp.where(place == 0, low, pltpu.roll(stack, 1, 1))
        high = jnp.where(has_high, pltpu.roll(s_hi, 15, 1), mirror)
        right = jnp.where(place == 15, high, pltpu.roll(stack, LANES - 1, 1))
        below, above, left, right = (lines_of(x) for x in (below, above, left, right))

        def whole(cells, direction):
            return along(cells, derived(cells), direction)

        mid = [along(ends, prims, d) for d in range(3)]
        c_up = twice_flux(mid[1], whole(above, 1), 1)
        c_dn = twice_flux(whole(below, 1), mid[1], 1)
        s_up = twice_flux(mid[2], whole(right, 2), 2)
        s_dn = twice_flux(whole(left, 2), mid[2], 2)
        other = [jnp.where(rotor, b, a) for a, b in zip(ends, nexts)]
        inner = [jnp.where(rotor, a, b) for a, b in zip(ends, nexts)]
        axial = twice_flux(whole(other, 0), whole(inner, 0), 0)
        sign = jnp.where(rotor, 1.0, -1.0)
        div = [
            (c_up[j] - c_dn[j]) + (s_up[j] - s_dn[j]) - sign * axial[j] for j in range(5)
        ]
        return advanced(ends, div, source(ends, force))

    def compact_finish(par, ends, base):
        turn = off_s[par]
        turn = jnp.where(rotor, turn, cycle - turn)
        start = lax.rem(circ * cd + turn - 1 + cycle, cycle)
        taps = [jnp.full((5, LANES), wts_s[par, k], F32) for k in range(4)]
        scale = 1.0 / ((taps[0] + taps[1]) + (taps[2] + taps[3]))
        ghost = jnp.zeros((5, LANES), F32)
        for k in range(4):
            place = start + k
            sector = lax.rem(place // cd, sectors)
            back = LANES - 16 * lax.rem(place, cd)
            turned = lax.rem(back, LANES)
            first = pltpu.roll(PR[par][sector], turned, 1)
            second = pltpu.roll(PR[par][lax.rem(sector + 1, sectors)], turned, 1)
            ghost = ghost + (taps[k] * scale) * jnp.where(lane < back, first, second)
        ghost = lines_of(ghost)
        left = [jnp.where(rotor, a, b) for a, b in zip(ends, ghost)]
        right = [jnp.where(rotor, b, a) for a, b in zip(ends, ghost)]
        plane = twice_flux(
            along(left, derived(left), 0), along(right, derived(right), 0), 0
        )
        step = jnp.where(rotor, -HALF_STEP, HALF_STEP)
        return plane, [base[j] + step * plane[j] for j in range(5)]

    def put_plane(par, plane):
        for j in range(5):
            PF[0, par, j] = to_tile(0.5 * plane[j])[:, :16]

    def insert(lines, dest):
        tile = jnp.broadcast_to(lines[0], (8, LANES))
        for f in range(1, 5):
            tile = jnp.where(sub8 == f, lines[f], tile)
        turned = jnp.transpose(tile)
        here = lax.broadcasted_iota(jnp.int32, (16, LANES), 1) == jnp.where(rotor, 127, 0)
        for f in range(5):
            for c in range(cd):
                column = jnp.broadcast_to(turned[16 * c : 16 * c + 16, f : f + 1], (16, LANES))
                dest(f, c, here, column)

    def prim_rows(par, first, last):
        def one(c, _):
            for h in range(2):
                values = derived([U[par, f, h, c] for f in range(5)])
                for k in range(5):
                    W[k, h, c] = values[k]
            return _

        lax.fori_loop(first, last, one, 0)

    lane16 = lax.broadcasted_iota(jnp.int32, (16, LANES), 1)
    sub16 = lax.broadcasted_iota(jnp.int32, (16, LANES), 0)

    def bulk(par, store):
        def state_at(c):
            return [
                ([U[par, f, h, c] for f in range(5)], [W[k, h, c] for k in range(5)])
                for h in range(2)
            ]

        def one(c, lower, last_row):
            here = state_at(c + 1)
            if last_row:
                upper = None
                div = [[-lower[h][j] for j in range(5)] for h in range(2)]
            else:
                there = state_at(c + 2)
                upper = tuple(
                    tuple(twice_flux(along(*here[h], 1), along(*there[h], 1), 1))
                    for h in range(2)
                )
                div = [[upper[h][j] - lower[h][j] for j in range(5)] for h in range(2)]

            full = [along(*here[h], 0) for h in range(2)]

            def before(pick, inlet):
                turned = [pltpu.roll(pick(full[h]), 1, 1) for h in range(2)]
                return (
                    jnp.where(lane16 == 0, inlet, turned[0]),
                    jnp.where(lane16 == 0, turned[0], turned[1]),
                )

            cells = [before(lambda s, f=f: s[0][f], INLET[f]) for f in range(5)]
            u = before(lambda s: s[1], INLET_U)
            p = before(lambda s: s[2], INLET_P)
            a = before(lambda s: s[3], INLET_U + INLET_SOUND)
            flux = [
                twice_flux(([x[h] for x in cells], u[h], p[h], a[h]), full[h], 0)
                for h in range(2)
            ]
            last = twice_flux(full[1], full[1], 0)
            for j in range(5):
                turned = [pltpu.roll(flux[h][j], LANES - 1, 1) for h in range(2)]
                div[0][j] += jnp.where(lane16 == 127, turned[1], turned[0]) - flux[0][j]
                div[1][j] += jnp.where(lane16 == 127, last[j], turned[1]) - flux[1][j]

            for h in range(2):
                full = along(*here[h], 2)
                flux = twice_flux(
                    (
                        [pltpu.roll(full[0][f], 1, 0) for f in range(5)],
                        pltpu.roll(full[1], 1, 0),
                        pltpu.roll(full[2], 1, 0),
                        pltpu.roll(full[3], 1, 0),
                    ),
                    full,
                    2,
                )
                for j in range(5):
                    inside = jnp.where(sub16 == 0, 0.0, flux[j])
                    div[h][j] += pltpu.roll(inside, 15, 0) - inside
                force = [FO[d, h, c] for d in range(3)]
                new = advanced(here[h][0], div[h], source(here[h][0], force))
                for j in range(5):
                    store(j, h, c, new[j])
            return upper

        none = jnp.zeros((16, LANES), F32)
        start = tuple(tuple(none for _ in range(5)) for _ in range(2))
        final = lax.fori_loop(0, cd - 1, lambda c, lower: one(c, lower, False), start)
        one(cd - 1, final, True)

    def edges(par, shift):
        def flux_of(low, high, direction):
            return twice_flux(
                along(low, derived(low), direction),
                along(high, derived(high), direction),
                direction,
            )

        for h in range(2):
            rows = [[U[par, f, h, c] for f in range(5)] for c in (0, 1, cd, cd + 1)]
            low = flux_of(rows[0], rows[1], 1)
            high = flux_of(rows[2], rows[3], 1)
            for j in range(5):
                shift(j, h, 0, pl.ds(0, 16), HALF_STEP * low[j])
                shift(j, h, cd - 1, pl.ds(0, 16), -HALF_STEP * high[j])
            bottom, top = ([SS[par, k, f, h] for f in range(5)] for k in (1, 0))
            below, above = ([SR[par, k, f, h] for f in range(5)] for k in (0, 1))
            low = flux_of(below, bottom, 2)
            high = flux_of(top, above, 2)
            for j in range(5):
                shift(j, h, pl.ds(0, cd), 0, HALF_STEP * low[j])
                shift(j, h, pl.ds(0, cd), 15, -HALF_STEP * high[j])

    def blocks_of(ref):
        return [ref(f).reshape(cd * 16, LANES) for f in range(5)]

    loaded(U.at[0, :, half, own], 0)
    (ends, nexts) = end_layers(blocks_of(lambda f: U[0, f, half, own]))

    def conserved(raw):
        r, v0, v1, v2, p = raw
        return [r, r * v0, r * v1, r * v2, p * 2.5 + 0.5 * r * (v0 * v0 + v1 * v1 + v2 * v2)]

    ends, nexts = conserved(ends), conserved(nexts)
    put_lines(0, ends)
    loaded(U.at[0, :, row, own], 1)
    loaded(FO, 2)
    load_offsets.wait()
    load_weights.wait()
    lax.fori_loop(1, cd + 1, conserve, 0)
    pack_span(0)
    force, _ = end_layers([FO[d, half].reshape(cd * 16, LANES) for d in range(3)])
    prim_rows(0, 1, cd + 1)
    peers = sectors + 2 + has_low.astype(jnp.int32) + has_high.astype(jnp.int32)
    pl.semaphore_wait(barrier, peers)
    for copy in plane_copies(0):
        copy.start()
    start_all(near_plane, 0)
    start_all(halo, 0)
    mirror_span(0)

    def keep(j, h, c, value):
        U[1, j, h, c + 1] = value

    bulk(0, keep)
    def shift_state(j, h, c, s, value):
        c = pl.ds(1, cd) if isinstance(c, pl.Slice) else c + 1
        U[1, j, h, c, s] = U[1, j, h, c, s] + value

    def halo_part():
        take_halos(0)
        edges(0, shift_state)
        drain_all(halo, 0)
        pack_span(1)
        for f in range(5):
            for h in range(2):
                SC[0, f, h] = U[1, f, h, cd]
                SC[1, f, h] = U[1, f, h, 1]
        start_all(halo, 1)
        mirror_span(1)

    take_planes(0)
    base = compact_base(0, ends, nexts, force)
    drain_all(near_plane, 0)
    all_planes(0).wait_recv()
    plane, ends = compact_finish(0, ends, base)
    put_lines(1, ends)
    start_all(near_plane, 1)
    for copy in plane_copies(1):
        copy.start()
    halo_part()
    put_plane(0, plane)

    def into_state(f, c, here, column):
        U[1, f, half, c + 1] = jnp.where(here, column, U[1, f, half, c + 1])

    insert(ends, into_state)

    _, nexts = end_layers(blocks_of(lambda f: U[1, f, half, own]))
    prim_rows(1, 1, cd + 1)

    def emit(j, h, c, value):
        OB[0, j, c, :, h * LANES : (h + 1) * LANES] = value

    bulk(1, emit)
    take_planes(1)
    base = compact_base(1, ends, nexts, force)
    take_halos(1)

    def shift_out(j, h, c, s, value):
        lanes = pl.ds(h * LANES, LANES)
        OB[0, j, c, s, lanes] = OB[0, j, c, s, lanes] + value

    edges(1, shift_out)
    all_planes(0).wait_send()
    all_planes(1).wait_send()
    drain_all(near_plane, 1)
    drain_all(halo, 1)
    all_planes(1).wait_recv()
    plane, ends = compact_finish(1, ends, base)

    def into_out(f, c, here, column):
        lanes = pl.ds(pl.multiple_of(half * LANES, LANES), LANES)
        OB[0, f, c, :, lanes] = jnp.where(here, column, OB[0, f, c, :, lanes])

    insert(ends, into_out)
    put_plane(1, plane)


def write_out(state, plane, out, plane_out, sems):
    writes = [
        pltpu.make_async_copy(state, out, sems.at[0]),
        pltpu.make_async_copy(plane, plane_out, sems.at[1]),
    ]
    for copy in writes:
        copy.start()
    for copy in writes:
        copy.wait()


def solution(mesh):
    sectors = mesh.shape["circ"]
    bands = mesh.shape["span"]

    def body(density, velocity, pressure, blade_force, offsets, weights):
        _, cd, sd, axial = density.shape
        vmem, dma = pltpu.VMEM, pltpu.SemaphoreType.DMA
        any_space = pl.BlockSpec(memory_space=pl.ANY)
        in_vmem = pl.BlockSpec(memory_space=pltpu.VMEM)
        results = pl.pallas_call(
            functools.partial(kernel, sectors, bands),
            out_shape=(
                vmem((1, 5, cd, sd, axial), F32),
                vmem((1, 2, 5, cd, sd), F32),
            ),
            in_specs=[any_space] * 6,
            out_specs=(in_vmem, in_vmem),
            scratch_shapes=[
                vmem((2, 5, 2, cd + 2, sd, LANES), F32),
                vmem((5, 2, cd + 2, sd, LANES), F32),
                vmem((3, 2, cd, sd, LANES), F32),
                vmem((2, 2, 5, 2, cd, LANES), F32),
                vmem((2, 2, 5, 2, cd, LANES), F32),
                vmem((2, 5, 2, sd, LANES), F32),
                vmem((2, 5, LANES), F32),
                vmem((sectors, 5, LANES), F32),
                vmem((sectors, 5, LANES), F32),
                vmem((2, 4, 5, LANES), F32),
                pltpu.SMEM((2,), jnp.int32),
                pltpu.SMEM((2, 4), F32),
                dma((10,)),
                dma((2,)),
                dma((2, 3)),
                dma((2, 4)),
            ],
            compiler_params=pltpu.CompilerParams(collective_id=0, has_side_effects=True),
        )(density, velocity, pressure, blade_force, offsets, weights)
        results = [pltpu.with_memory_space_constraint(x, pltpu.VMEM) for x in results]
        return pl.pallas_call(
            write_out,
            out_shape=(
                jax.ShapeDtypeStruct((1, 5, cd, sd, axial), F32),
                jax.ShapeDtypeStruct((1, 2, 5, cd, sd), F32),
            ),
            in_specs=[in_vmem, in_vmem],
            out_specs=(any_space, any_space),
            scratch_shapes=[dma((2,))],
        )(*results)

    placed = (
        P("row", "circ", "span", None),
        P("row", None, "circ", "span", None),
        P("row", "circ", "span", None),
        P("row", None, "circ", "span", None),
        P(),
        P(),
    )
    return jax.shard_map(
        body,
        mesh=mesh,
        in_specs=placed,
        out_specs=(P("row", None, "circ", "span", None), P("row", None, None, "circ", "span")),
        check_vma=False,
    )
```

```python
import functools
import math

import jax
import jax.numpy as jnp
from jax import lax
from jax.experimental import pallas as pl
from jax.experimental.pallas import tpu as pltpu
from jax.sharding import PartitionSpec as P

F32 = jnp.float32
MESH = pl.DeviceIdType.MESH
TIME_STEP = 0.04
HALF_STEP = 0.5 * TIME_STEP
LANES = 128
INLET = (1.0, 0.5, 0.0, 0.0, 2.625)
INLET_U = 0.5
INLET_P = 1.0
INLET_SOUND = math.sqrt(1.4)


def derived(cells):
    density, m0, m1, m2, energy = cells
    inverse = 1.0 / density
    u0, u1, u2 = m0 * inverse, m1 * inverse, m2 * inverse
    pressure = 0.4 * (energy - 0.5 * (m0 * u0 + m1 * u1 + m2 * u2))
    sound = jnp.sqrt(1.4 * pressure * inverse)
    return (u0, u1, u2, pressure, sound)


def twice_flux(left, right, direction):
    cells_l, u_l, p_l, a_l = left
    cells_r, u_r, p_r, a_r = right
    speed = jnp.maximum(a_l, a_r)
    up, down = u_l + speed, u_r - speed
    out = [cells_l[j] * up + cells_r[j] * down for j in range(5)]
    out[1 + direction] = out[1 + direction] + (p_l + p_r)
    out[4] = out[4] + (p_l * u_l + p_r * u_r)
    return out


def along(cells, prims, direction):
    normal = prims[direction]
    return (cells, normal, prims[3], jnp.abs(normal) + prims[4])


def source(cells, force):
    return [
        None,
        cells[0] * force[0],
        cells[0] * force[1],
        cells[0] * force[2],
        cells[1] * force[0] + cells[2] * force[1] + cells[3] * force[2],
    ]


def advanced(cells, div, src):
    out = []
    for j in range(5):
        value = cells[j] - HALF_STEP * div[j]
        if src[j] is not None:
            value = value + TIME_STEP * src[j]
        out.append(value)
    return out


def kernel(
    sectors,
    bands,
    dens,
    vel,
    pres,
    forc,
    offs,
    wts,
    OB,
    PF,
    U,
    W,
    FO,
    SS,
    SR,
    SC,
    PS,
    PR0,
    PR1,
    PN,
    off_s,
    wts_s,
    local_sem,
    pr_sem,
    nr_sem,
    hr_sem,
):
    row = lax.axis_index("row")
    circ = lax.axis_index("circ")
    span = lax.axis_index("span")
    cd = FO.shape[2]
    cycle = sectors * cd
    c_low, c_high = lax.rem(circ + sectors - 1, sectors), lax.rem(circ + 1, sectors)
    has_low, has_high = span > 0, span < bands - 1
    rotor = row == 0
    half = 1 - row

    own = pl.ds(1, cd)
    PR = (PR0, PR1)

    def load_half(h, sem):
        lanes = pl.ds(pl.multiple_of(h * LANES, LANES), LANES)
        for src, dst in (
            (dens.at[0, :, :, lanes], U.at[0, 0, h, own]),
            (vel.at[0, :, :, :, lanes], U.at[0, pl.ds(1, 3), h, own]),
            (pres.at[0, :, :, lanes], U.at[0, 4, h, own]),
        ):
            pltpu.make_async_copy(src, dst, local_sem.at[sem]).start()

    def loaded(ref, sem):
        pltpu.make_async_copy(ref, ref, local_sem.at[sem]).wait()

    load_half(half, 0)
    barrier = pltpu.get_barrier_semaphore()
    for i in range(sectors):
        q = lax.rem(circ + sectors // 2 + i, sectors)
        pl.semaphore_signal(
            barrier, inc=1, device_id={"row": 1 - row, "circ": q}, device_id_type=MESH
        )
    for q in (c_low, c_high):
        pl.semaphore_signal(barrier, inc=1, device_id={"circ": q}, device_id_type=MESH)

    @pl.when(has_low)
    def _():
        pl.semaphore_signal(barrier, inc=1, device_id={"span": span - 1}, device_id_type=MESH)

    @pl.when(has_high)
    def _():
        pl.semaphore_signal(barrier, inc=1, device_id={"span": span + 1}, device_id_type=MESH)

    load_half(row, 1)
    for h in range(2):
        lanes = pl.ds(h * LANES, LANES)
        pltpu.make_async_copy(forc.at[0, :, :, :, lanes], FO.at[:, h], local_sem.at[2]).start()
    load_offsets = pltpu.make_async_copy(offs, off_s, local_sem.at[3])
    load_weights = pltpu.make_async_copy(wts, wts_s, local_sem.at[4])
    load_offsets.start()
    load_weights.start()

    lane = lax.broadcasted_iota(jnp.int32, (5, LANES), 1)
    sub8 = lax.broadcasted_iota(jnp.int32, (8, LANES), 0)

    def conserve(c, _):
        for h in range(2):
            r = U[0, 0, h, c]
            v = [U[0, 1 + d, h, c] for d in range(3)]
            p = U[0, 4, h, c]
            for d in range(3):
                U[0, 1 + d, h, c] = r * v[d]
            U[0, 4, h, c] = p * 2.5 + 0.5 * r * (v[0] * v[0] + v[1] * v[1] + v[2] * v[2])
        return _

    def to_tile(line):
        tile = jnp.broadcast_to(line, (8, LANES))
        for bit in (4, 2, 1):
            tile = jnp.where((sub8 & bit) != 0, pltpu.roll(tile, LANES - 16 * bit, 1), tile)
        return tile

    def end_layers(block_of):
        ends, nexts = [], []
        for turned in (jnp.transpose(b) for b in block_of):
            ends.append(jnp.where(rotor, turned[127:128], turned[0:1]))
            nexts.append(jnp.where(rotor, turned[126:127], turned[1:2]))
        return ends, nexts

    def put_lines(par, lines):
        for f in range(5):
            PS[par, f : f + 1] = lines[f]

    def lines_of(stack):
        return [stack[f : f + 1] for f in range(5)]

    def plane_copies(par):
        copies = []
        for i in range(sectors):
            q = lax.rem(circ + sectors // 2 + i, sectors)
            copies.append(
                pltpu.make_async_remote_copy(
                    src_ref=PS.at[par],
                    dst_ref=PR[par].at[circ],
                    send_sem=local_sem.at[par],
                    recv_sem=pr_sem.at[par],
                    device_id={"row": 1 - row, "circ": q},
                    device_id_type=MESH,
                )
            )
        return copies

    def all_planes(par):
        return pltpu.make_async_remote_copy(
            src_ref=PR[par],
            dst_ref=PR[par],
            send_sem=local_sem.at[par],
            recv_sem=pr_sem.at[par],
            device_id={"row": 1 - row},
            device_id_type=MESH,
        )

    def to_neighbour(side, src, dst, send_sem, recv_sem):
        where = (
            {"circ": c_high},
            {"circ": c_low},
            {"span": span + 1},
            {"span": span - 1},
        )[side]
        return pltpu.make_async_remote_copy(
            src_ref=src,
            dst_ref=dst,
            send_sem=send_sem,
            recv_sem=recv_sem,
            device_id=where,
            device_id_type=MESH,
        )

    def near_plane(par, side):
        return to_neighbour(
            side, PS.at[par], PN.at[par, side], local_sem.at[2 + side], nr_sem.at[par, max(side - 1, 0)]
        )

    def halo(par, side):
        if side < 2:
            src = SC.at[side] if par else U.at[par, :, :, cd if side == 0 else 1]
            dst = U.at[par, :, :, 0 if side == 0 else cd + 1]
        else:
            src, dst = SS.at[par, side - 2], SR.at[par, side - 2]
        return to_neighbour(side, src, dst, local_sem.at[6 + side], hr_sem.at[par, side])

    sends = (None, None, has_high, has_low)
    takes = (None, None, has_low, has_high)

    def guarded(condition, act):
        if condition is None:
            act()
        else:
            pl.when(condition)(act)

    def start_all(make, par, sides=range(4)):
        for side in sides:
            guarded(sends[side], lambda side=side: make(par, side).start())

    def take_planes(par):
        both = pltpu.make_async_remote_copy(
            src_ref=PN.at[par, pl.ds(0, 2)],
            dst_ref=PN.at[par, pl.ds(0, 2)],
            send_sem=local_sem.at[2],
            recv_sem=nr_sem.at[par, 0],
            device_id={"circ": c_low},
            device_id_type=MESH,
        )
        both.wait_recv()
        for side in (2, 3):
            guarded(takes[side], lambda side=side: near_plane(par, side).wait_recv())

    def take_halos(par):
        for side in range(4):
            guarded(takes[side], lambda side=side: halo(par, side).wait_recv())

    def drain_all(make, par):
        for side in range(4):
            guarded(sends[side], lambda side=side: make(par, side).wait_send())

    def pack_span(par):
        for f in range(5):
            for h in range(2):
                cells = U[par, f, h, own]
                SS[par, 0, f, h] = cells[:, 15]
                SS[par, 1, f, h] = cells[:, 0]

    def mirror_span(par):
        def hub():
            for f in range(5):
                for h in range(2):
                    edge = SS[par, 1, f, h]
                    SR[par, 0, f, h] = -edge if f == 3 else edge

        def casing():
            for f in range(5):
                for h in range(2):
                    edge = SS[par, 0, f, h]
                    SR[par, 1, f, h] = -edge if f == 3 else edge

        pl.when(jnp.logical_not(has_low))(hub)
        pl.when(jnp.logical_not(has_high))(casing)

    def compact_base(par, ends, nexts, force):
        prims = derived(ends)
        stack = PS[par]
        c_lo, c_hi, s_lo, s_hi = (PN[par, k] for k in range(4))
        field = lax.broadcasted_iota(jnp.int32, (5, LANES), 0)
        mirror = jnp.where(field == 3, -stack, stack)
        place = lane % 16
        below = pltpu.roll(jnp.where(lane >= LANES - 16, c_lo, stack), 16, 1)
        above = pltpu.roll(jnp.where(lane < 16, c_hi, stack), LANES - 16, 1)
        low = jnp.where(has_low, pltpu.roll(s_lo, LANES - 15, 1), mirror)
        left = jnp.where(place == 0, low, pltpu.roll(stack, 1, 1))
        high = jnp.where(has_high, pltpu.roll(s_hi, 15, 1), mirror)
        right = jnp.where(place == 15, high, pltpu.roll(stack, LANES - 1, 1))
        below, above, left, right = (lines_of(x) for x in (below, above, left, right))

        def whole(cells, direction):
            return along(cells, derived(cells), direction)

        mid = [along(ends, prims, d) for d in range(3)]
        c_up = twice_flux(mid[1], whole(above, 1), 1)
        c_dn = twice_flux(whole(below, 1), mid[1], 1)
        s_up = twice_flux(mid[2], whole(right, 2), 2)
        s_dn = twice_flux(whole(left, 2), mid[2], 2)
        other = [jnp.where(rotor, b, a) for a, b in zip(ends, nexts)]
        inner = [jnp.where(rotor, a, b) for a, b in zip(ends, nexts)]
        axial = twice_flux(whole(other, 0), whole(inner, 0), 0)
        sign = jnp.where(rotor, 1.0, -1.0)
        div = [
            (c_up[j] - c_dn[j]) + (s_up[j] - s_dn[j]) - sign * axial[j] for j in range(5)
        ]
        return advanced(ends, div, source(ends, force))

    def compact_finish(par, ends, base):
        turn = off_s[par]
        turn = jnp.where(rotor, turn, cycle - turn)
        start = lax.rem(circ * cd + turn - 1 + cycle, cycle)
        taps = [jnp.full((5, LANES), wts_s[par, k], F32) for k in range(4)]
        scale = 1.0 / ((taps[0] + taps[1]) + (taps[2] + taps[3]))
        ghost = jnp.zeros((5, LANES), F32)
        for k in range(4):
            place = start + k
            sector = lax.rem(place // cd, sectors)
            back = LANES - 16 * lax.rem(place, cd)
            turned = lax.rem(back, LANES)
            first = pltpu.roll(PR[par][sector], turned, 1)
            second = pltpu.roll(PR[par][lax.rem(sector + 1, sectors)], turned, 1)
            ghost = ghost + (taps[k] * scale) * jnp.where(lane < back, first, second)
        ghost = lines_of(ghost)
        left = [jnp.where(rotor, a, b) for a, b in zip(ends, ghost)]
        right = [jnp.where(rotor, b, a) for a, b in zip(ends, ghost)]
        plane = twice_flux(
            along(left, derived(left), 0), along(right, derived(right), 0), 0
        )
        step = jnp.where(rotor, -HALF_STEP, HALF_STEP)
        return plane, [base[j] + step * plane[j] for j in range(5)]

    def put_plane(par, plane):
        for j in range(5):
            PF[0, par, j] = to_tile(0.5 * plane[j])[:, :16]

    def insert(lines, dest):
        tile = jnp.broadcast_to(lines[0], (8, LANES))
        for f in range(1, 5):
            tile = jnp.where(sub8 == f, lines[f], tile)
        turned = jnp.transpose(tile)
        here = lax.broadcasted_iota(jnp.int32, (16, LANES), 1) == jnp.where(rotor, 127, 0)
        for f in range(5):
            for c in range(cd):
                column = jnp.broadcast_to(turned[16 * c : 16 * c + 16, f : f + 1], (16, LANES))
                dest(f, c, here, column)

    def prim_rows(par, first, last):
        def one(c, _):
            for h in range(2):
                values = derived([U[par, f, h, c] for f in range(5)])
                for k in range(5):
                    W[k, h, c] = values[k]
            return _

        lax.fori_loop(first, last, one, 0)

    lane16 = lax.broadcasted_iota(jnp.int32, (16, LANES), 1)
    sub16 = lax.broadcasted_iota(jnp.int32, (16, LANES), 0)

    def bulk(par, store):
        def state_at(c):
            return [
                ([U[par, f, h, c] for f in range(5)], [W[k, h, c] for k in range(5)])
                for h in range(2)
            ]

        def one(c, lower, last_row):
            here = state_at(c + 1)
            if last_row:
                upper = None
                div = [[-lower[h][j] for j in range(5)] for h in range(2)]
            else:
                there = state_at(c + 2)
                upper = tuple(
                    tuple(twice_flux(along(*here[h], 1), along(*there[h], 1), 1))
                    for h in range(2)
                )
                div = [[upper[h][j] - lower[h][j] for j in range(5)] for h in range(2)]

            full = [along(*here[h], 0) for h in range(2)]

            def before(pick, inlet):
                turned = [pltpu.roll(pick(full[h]), 1, 1) for h in range(2)]
                return (
                    jnp.where(lane16 == 0, inlet, turned[0]),
                    jnp.where(lane16 == 0, turned[0], turned[1]),
                )

            cells = [before(lambda s, f=f: s[0][f], INLET[f]) for f in range(5)]
            u = before(lambda s: s[1], INLET_U)
            p = before(lambda s: s[2], INLET_P)
            a = before(lambda s: s[3], INLET_U + INLET_SOUND)
            flux = [
                twice_flux(([x[h] for x in cells], u[h], p[h], a[h]), full[h], 0)
                for h in range(2)
            ]
            last = twice_flux(full[1], full[1], 0)
            for j in range(5):
                turned = [pltpu.roll(flux[h][j], LANES - 1, 1) for h in range(2)]
                div[0][j] += jnp.where(lane16 == 127, turned[1], turned[0]) - flux[0][j]
                div[1][j] += jnp.where(lane16 == 127, last[j], turned[1]) - flux[1][j]

            for h in range(2):
                full = along(*here[h], 2)
                flux = twice_flux(
                    (
                        [pltpu.roll(full[0][f], 1, 0) for f in range(5)],
                        pltpu.roll(full[1], 1, 0),
                        pltpu.roll(full[2], 1, 0),
                        pltpu.roll(full[3], 1, 0),
                    ),
                    full,
                    2,
                )
                for j in range(5):
                    inside = jnp.where(sub16 == 0, 0.0, flux[j])
                    div[h][j] += pltpu.roll(inside, 15, 0) - inside
                force = [FO[d, h, c] for d in range(3)]
                new = advanced(here[h][0], div[h], source(here[h][0], force))
                for j in range(5):
                    store(j, h, c, new[j])
            return upper

        none = jnp.zeros((16, LANES), F32)
        start = tuple(tuple(none for _ in range(5)) for _ in range(2))
        final = lax.fori_loop(0, cd - 1, lambda c, lower: one(c, lower, False), start)
        one(cd - 1, final, True)

    def edges(par, shift):
        def flux_of(low, high, direction):
            return twice_flux(
                along(low, derived(low), direction),
                along(high, derived(high), direction),
                direction,
            )

        for h in range(2):
            rows = [[U[par, f, h, c] for f in range(5)] for c in (0, 1, cd, cd + 1)]
            low = flux_of(rows[0], rows[1], 1)
            high = flux_of(rows[2], rows[3], 1)
            for j in range(5):
                shift(j, h, 0, pl.ds(0, 16), HALF_STEP * low[j])
                shift(j, h, cd - 1, pl.ds(0, 16), -HALF_STEP * high[j])
            bottom, top = ([SS[par, k, f, h] for f in range(5)] for k in (1, 0))
            below, above = ([SR[par, k, f, h] for f in range(5)] for k in (0, 1))
            low = flux_of(below, bottom, 2)
            high = flux_of(top, above, 2)
            for j in range(5):
                shift(j, h, pl.ds(0, cd), 0, HALF_STEP * low[j])
                shift(j, h, pl.ds(0, cd), 15, -HALF_STEP * high[j])

    def blocks_of(ref):
        return [ref(f).reshape(cd * 16, LANES) for f in range(5)]

    loaded(U.at[0, :, half, own], 0)
    (ends, nexts) = end_layers(blocks_of(lambda f: U[0, f, half, own]))

    def conserved(raw):
        r, v0, v1, v2, p = raw
        return [r, r * v0, r * v1, r * v2, p * 2.5 + 0.5 * r * (v0 * v0 + v1 * v1 + v2 * v2)]

    ends, nexts = conserved(ends), conserved(nexts)
    put_lines(0, ends)
    loaded(U.at[0, :, row, own], 1)
    loaded(FO, 2)
    load_offsets.wait()
    load_weights.wait()
    lax.fori_loop(1, cd + 1, conserve, 0)
    pack_span(0)
    force, _ = end_layers([FO[d, half].reshape(cd * 16, LANES) for d in range(3)])
    prim_rows(0, 1, cd + 1)
    peers = sectors + 2 + has_low.astype(jnp.int32) + has_high.astype(jnp.int32)
    pl.semaphore_wait(barrier, peers)
    for copy in plane_copies(0):
        copy.start()
    start_all(near_plane, 0)
    start_all(halo, 0)
    mirror_span(0)

    def keep(j, h, c, value):
        U[1, j, h, c + 1] = value

    bulk(0, keep)
    def shift_state(j, h, c, s, value):
        c = pl.ds(1, cd) if isinstance(c, pl.Slice) else c + 1
        U[1, j, h, c, s] = U[1, j, h, c, s] + value

    def halo_part():
        take_halos(0)
        edges(0, shift_state)
        drain_all(halo, 0)
        for f in range(5):
            for h in range(2):
                SC[0, f, h] = U[1, f, h, cd]
                SC[1, f, h] = U[1, f, h, 1]
        start_all(halo, 1, (0, 1))
        pack_span(1)
        start_all(halo, 1, (2, 3))
        mirror_span(1)

    take_planes(0)
    base = compact_base(0, ends, nexts, force)
    drain_all(near_plane, 0)
    all_planes(0).wait_recv()
    plane, ends = compact_finish(0, ends, base)
    put_lines(1, ends)
    start_all(near_plane, 1)
    for copy in plane_copies(1):
        copy.start()
    halo_part()
    put_plane(0, plane)

    def into_state(f, c, here, column):
        U[1, f, half, c + 1] = jnp.where(here, column, U[1, f, half, c + 1])

    insert(ends, into_state)

    _, nexts = end_layers(blocks_of(lambda f: U[1, f, half, own]))
    prim_rows(1, 1, cd + 1)

    def emit(j, h, c, value):
        OB[0, j, c, :, h * LANES : (h + 1) * LANES] = value

    bulk(1, emit)
    take_planes(1)
    base = compact_base(1, ends, nexts, force)
    take_halos(1)

    def shift_out(j, h, c, s, value):
        lanes = pl.ds(h * LANES, LANES)
        OB[0, j, c, s, lanes] = OB[0, j, c, s, lanes] + value

    edges(1, shift_out)
    all_planes(0).wait_send()
    all_planes(1).wait_send()
    drain_all(near_plane, 1)
    drain_all(halo, 1)
    all_planes(1).wait_recv()
    plane, ends = compact_finish(1, ends, base)

    def into_out(f, c, here, column):
        lanes = pl.ds(pl.multiple_of(half * LANES, LANES), LANES)
        OB[0, f, c, :, lanes] = jnp.where(here, column, OB[0, f, c, :, lanes])

    insert(ends, into_out)
    put_plane(1, plane)


def write_out(state, plane, out, plane_out, sems):
    writes = [
        pltpu.make_async_copy(state, out, sems.at[0]),
        pltpu.make_async_copy(plane, plane_out, sems.at[1]),
    ]
    for copy in writes:
        copy.start()
    for copy in writes:
        copy.wait()


def solution(mesh):
    sectors = mesh.shape["circ"]
    bands = mesh.shape["span"]

    def body(density, velocity, pressure, blade_force, offsets, weights):
        _, cd, sd, axial = density.shape
        vmem, dma = pltpu.VMEM, pltpu.SemaphoreType.DMA
        any_space = pl.BlockSpec(memory_space=pl.ANY)
        in_vmem = pl.BlockSpec(memory_space=pltpu.VMEM)
        results = pl.pallas_call(
            functools.partial(kernel, sectors, bands),
            out_shape=(
                vmem((1, 5, cd, sd, axial), F32),
                vmem((1, 2, 5, cd, sd), F32),
            ),
            in_specs=[any_space] * 6,
            out_specs=(in_vmem, in_vmem),
            scratch_shapes=[
                vmem((2, 5, 2, cd + 2, sd, LANES), F32),
                vmem((5, 2, cd + 2, sd, LANES), F32),
                vmem((3, 2, cd, sd, LANES), F32),
                vmem((2, 2, 5, 2, cd, LANES), F32),
                vmem((2, 2, 5, 2, cd, LANES), F32),
                vmem((2, 5, 2, sd, LANES), F32),
                vmem((2, 5, LANES), F32),
                vmem((sectors, 5, LANES), F32),
                vmem((sectors, 5, LANES), F32),
                vmem((2, 4, 5, LANES), F32),
                pltpu.SMEM((2,), jnp.int32),
                pltpu.SMEM((2, 4), F32),
                dma((10,)),
                dma((2,)),
                dma((2, 3)),
                dma((2, 4)),
            ],
            compiler_params=pltpu.CompilerParams(collective_id=0, has_side_effects=True),
        )(density, velocity, pressure, blade_force, offsets, weights)
        results = [pltpu.with_memory_space_constraint(x, pltpu.VMEM) for x in results]
        return pl.pallas_call(
            write_out,
            out_shape=(
                jax.ShapeDtypeStruct((1, 5, cd, sd, axial), F32),
                jax.ShapeDtypeStruct((1, 2, 5, cd, sd), F32),
            ),
            in_specs=[in_vmem, in_vmem],
            out_specs=(any_space, any_space),
            scratch_shapes=[dma((2,))],
        )(*results)

    placed = (
        P("row", "circ", "span", None),
        P("row", None, "circ", "span", None),
        P("row", "circ", "span", None),
        P("row", None, "circ", "span", None),
        P(),
        P(),
    )
    return jax.shard_map(
        body,
        mesh=mesh,
        in_specs=placed,
        out_specs=(P("row", None, "circ", "span", None), P("row", None, None, "circ", "span")),
        check_vma=False,
    )
```
